32 devices in a mesh: group: 4 (over y, core), peer: 8 (over z, x).
Axes of the slice: x: 2, y: 2, z: 4, core: 2. Of those that a mesh axis runs over, the one named last changes fastest.
Arguments:
- states: float32 [41, 1048576], P(None, ('group', 'peer')), may hold values from -6 to 6
- block_part: int32 [8192], P(('group', 'peer')), may hold values from 0 to 31, as said below
- tile_perm: int32 [8192, 128], P(('group', 'peer')), may hold values from 0 to 127, each once within a row
- half_volt: float32 [40], replicated, may hold values from -4 to 4
- steepness: float32 [40], replicated, may hold values from 0.5 to 4
- gate_rate: float32 [40], replicated, may hold values from 0.1 to 1
- conductance: float32 [40], replicated, may hold values from 0.005 to 0.08
- reversal: float32 [40], replicated, may hold values from -6 to 6
Outputs:
- regrouped: float32 [41, 1048576], P(None, ('group', 'peer'))
The draws below stay inside these ranges and needn't reach their ends.
Inputs may be any that keep to these rules, and one draw needn't show every extreme that they name: `block_part`: every partition holds exactly 256 blocks. Within each slab of 256 consecutive global blocks no partition holds more than 16 blocks; every slab has exactly 16 blocks of some partition, and every partition has exactly 16 blocks in some slab.
All inputs are finite; a program needn't handle non-finite values.
Results may differ from the reference program's by a relative error of at most 0.0001.
Values sent between devices are 32-bit elements; how exact they have to be, the bound alone decides.
A program may use at most 192 MiB of HBM per device.

```python
import math
import jax
import jax.numpy as jnp
from jax import lax

STATES = 41
NODE_BLK = 128
BLK_DEV = 256
SUBSTEPS = 1
GATES = 40
BLOCKS = 8192
NODES = 1048576


def draw_block_part(key, part):
    devices = BLOCKS // BLK_DEV
    mean_count = BLK_DEV // devices
    pair_count = devices // 2
    key_order = jax.random.fold_in(key, 11)
    key_amount = jax.random.fold_in(key, 12)
    key_shuffle = jax.random.fold_in(key, 13)
    ordering = jax.random.permutation(key_order, devices).astype(jnp.int32)
    amounts = jax.random.randint(key_amount, (pair_count,), -mean_count, mean_count + 1, dtype=jnp.int32)
    amounts = amounts.at[0].set(mean_count)
    row_ids = jnp.arange(devices, dtype=jnp.int32)
    pair_ids = jnp.arange(pair_count, dtype=jnp.int32)
    plus_cols = ordering[(row_ids[:, None] + 2 * pair_ids[None, :]) % devices]
    minus_cols = ordering[(row_ids[:, None] + 2 * pair_ids[None, :] + 1) % devices]
    row_grid = jnp.broadcast_to(row_ids[:, None], (devices, pair_count))
    amount_grid = jnp.broadcast_to(amounts[None, :], (devices, pair_count))
    counts = jnp.full((devices, devices), mean_count, jnp.int32)
    counts = counts.at[row_grid, plus_cols].add(amount_grid)
    counts = counts.at[row_grid, minus_cols].add(-amount_grid)
    running = jnp.cumsum(counts, axis=1, dtype=jnp.int32)
    position = jnp.arange(BLK_DEV, dtype=jnp.int32)
    labels = jnp.sum((running[:, None, :] <= position[None, :, None]).astype(jnp.int32), axis=2, dtype=jnp.int32)
    row_keys = jax.random.split(key_shuffle, devices)
    shuffled = jax.vmap(lambda row_key, row_vals: jax.random.permutation(row_key, row_vals))(row_keys, labels)
    return shuffled.reshape(-1).astype(jnp.int32)


def level_of(own_key, extent, cuts, low, largest):
    gain = 1.0
    for dim, parts in cuts:
        steps = jax.random.uniform(jax.random.fold_in(jax.random.fold_in(own_key, 6), dim), (parts,), jnp.float32, low / len(cuts), largest / len(cuts))
        gain = gain * jnp.repeat(jnp.exp(steps), extent[dim] // parts).reshape((-1,) + (1,) * (len(extent) - 1 - dim))
    return gain


def normal_values(stream_key, dims, width, reach, shards=(), kind=jnp.bfloat16):
    result = width * jax.random.normal(stream_key, dims, jnp.float32)
    if shards:
        result = result * level_of(stream_key, dims, shards, -0.22, 0.18)
    return jnp.clip(result, -reach, reach).astype(kind)


def setup_inputs(seed: int = 0) -> dict:
    key_list = jax.random.split(jax.random.key(seed), 9)
    return {
        "states": normal_values(key_list[0], (STATES, NODES), 1.0, 6.0, ((1, 32),), jnp.float32),
        "block_part": draw_block_part(jax.random.fold_in(key_list[8], 71), 0),
        "tile_perm": jax.vmap(lambda own: jax.random.permutation(own, NODE_BLK))(jax.random.split(key_list[2], BLOCKS)).reshape((BLOCKS, NODE_BLK)).astype(jnp.int32),
        "half_volt": normal_values(key_list[3], (GATES,), 1.0, 4.0, (), jnp.float32),
        "steepness": jnp.clip(jnp.exp(jax.random.uniform(key_list[4], (GATES,), jnp.float32, math.log(0.5), math.log(4.0))), 0.5, 4.0),
        "gate_rate": jnp.clip(jnp.exp(jax.random.uniform(key_list[5], (GATES,), jnp.float32, math.log(0.1), math.log(1.0))), 0.1, 1.0),
        "conductance": jnp.clip(jnp.exp(jax.random.uniform(key_list[6], (GATES,), jnp.float32, math.log(0.005), math.log(0.08))), 0.005, 0.08),
        "reversal": normal_values(key_list[7], (GATES,), 1.5, 6.0, (), jnp.float32),
    }


time_step = 0.25


def advance(state_rows, half_volt, steepness, gate_rate, conductance, reversal):
    voltage = state_rows[0:1]
    gate_vals = state_rows[1:]
    for substep in range(SUBSTEPS):
        steady = jax.nn.sigmoid((voltage - half_volt[:, None]) * steepness[:, None])
        damping = jnp.exp(-gate_rate[:, None] * (1.0 + jax.nn.sigmoid(voltage)))
        gate_vals = steady + (gate_vals - steady) * damping
        current = jnp.sum(conductance[:, None] * gate_vals * (voltage - reversal[:, None]), axis=0, keepdims=True)
        voltage = voltage - time_step * current
    return jnp.concatenate([voltage, gate_vals], axis=0)


def reference(states, block_part, tile_perm, half_volt, steepness, gate_rate, conductance, reversal):
    devices = BLOCKS // BLK_DEV
    span = BLK_DEV * NODE_BLK

    def one_part(index, acc):
        start = (index * span).astype(jnp.int32)
        piece = lax.dynamic_slice_in_dim(states, start, span, 1)
        done = advance(piece, half_volt, steepness, gate_rate, conductance, reversal)
        return lax.dynamic_update_slice_in_dim(acc, done, start, 1)

    advanced = lax.fori_loop(0, devices, one_part, jnp.zeros_like(states))
    ordering = jnp.argsort(block_part, stable=True).astype(jnp.int32)
    local_index = jnp.zeros((BLOCKS,), jnp.int32).at[ordering].set(jnp.arange(BLOCKS, dtype=jnp.int32))
    columns = (local_index[:, None] * NODE_BLK + tile_perm).reshape(-1).astype(jnp.int32)
    return jnp.take(advanced, columns, axis=1)
```

```python
import functools
import jax
import jax.numpy as jnp
import numpy as np
from jax import lax
from jax.experimental import pallas as pl
from jax.experimental.pallas import tpu as pltpu
from jax.sharding import PartitionSpec as P

time_step = 0.25
LANES = 128
ROWS = 8
MESH_ID = pl.DeviceIdType.MESH
VMEM_LIMIT = 67043328
Z_STRIDE = 88
Z_NEAR = 88
P_STRIDE = 48
P_TABLE = 64
TIERS = ((72, 40), (80, 40), (88, 48))


def my_index(peers):
    return lax.axis_index("group") * peers + lax.axis_index("peer")


def counts_kernel(devices, peers, x_ref, out_ref, send_sem, recv_sem, local_sem):
    d = my_index(peers)
    barrier = pltpu.get_barrier_semaphore()
    for k in range(1, devices):
        to = (d + k) % devices
        pl.semaphore_signal(
            barrier, inc=1, device_id=(to // peers, to % peers), device_id_type=MESH_ID
        )
    pl.semaphore_wait(barrier, devices - 1)
    own = pltpu.make_async_copy(x_ref.at[0], out_ref.at[d], local_sem)
    own.start()
    for k in range(1, devices):
        to = (d + k) % devices
        pltpu.make_async_remote_copy(
            src_ref=x_ref.at[0], dst_ref=out_ref.at[d],
            send_sem=send_sem.at[k], recv_sem=recv_sem.at[k],
            device_id=(to // peers, to % peers), device_id_type=MESH_ID,
        ).start()
    own.wait()
    for k in range(1, devices):
        src = (d + devices - k) % devices
        pltpu.make_async_remote_copy(
            src_ref=x_ref.at[0], dst_ref=out_ref.at[src],
            send_sem=send_sem.at[k], recv_sem=recv_sem.at[k],
            device_id=(src // peers, src % peers), device_id_type=MESH_ID,
        ).wait()


def gather_counts(row, devices, peers):
    return pl.pallas_call(
        functools.partial(counts_kernel, devices, peers),
        out_shape=jax.ShapeDtypeStruct((devices, 1, LANES), jnp.int32),
        in_specs=[pl.BlockSpec(memory_space=pltpu.VMEM)],
        out_specs=pl.BlockSpec(memory_space=pltpu.VMEM),
        scratch_shapes=[
            pltpu.SemaphoreType.DMA((devices,)),
            pltpu.SemaphoreType.DMA((devices,)),
            pltpu.SemaphoreType.DMA,
        ],
        compiler_params=pltpu.CompilerParams(collective_id=0, has_side_effects=True),
    )(row)


def plane_of(d, peers):
    return (d // peers) * 2 + d % 2


def depth_of(d, peers):
    return (d % peers) // 2


def dot(a, b, contract=((1,), (0,))):
    return lax.dot_general(
        a, b, (contract, ((), ())), preferred_element_type=jnp.float32
    )


def iota(shape, axis):
    return lax.broadcasted_iota(jnp.int32, shape, axis)


def table_kernel(devices, peers, own_blocks, c_ref, part_ref, tab_ref, tier_ref):
    d = my_index(peers)
    plane = plane_of(d, peers)
    depth = depth_of(d, peers)
    planes = ROWS
    depths = peers // 2
    per = own_blocks // planes
    f32 = jnp.float32
    shift = ROWS - 1
    counts = c_ref[...].reshape(devices, LANES)
    lower = (iota((devices, devices), 1) < iota((devices, devices), 0)).astype(f32)
    starts = dot(lower, counts.astype(f32))
    starts_i = starts.astype(jnp.int32)
    upper = (
        iota((own_blocks, own_blocks), 0) < iota((own_blocks, own_blocks), 1)
    ).astype(f32)
    lane = iota((1, own_blocks), 1)
    lane_plane = lane // per
    stored = (lane % per) * planes + (plane ^ lane_plane)
    source_rows = iota((LANES, own_blocks), 0)
    row8 = iota((ROWS, own_blocks), 0)

    def classify(level):
        source = (lane_plane // 2) * peers + level * 2 + lane_plane % 2
        pick = (source_rows == source).astype(f32)
        begin = dot(starts, pick).astype(jnp.int32)
        dest = jnp.sum((begin <= stored).astype(jnp.int32), axis=0, keepdims=True) - 1
        level_to = depth_of(dest, peers)
        mask = (row8 == level_to).astype(f32)
        rank = jnp.sum(mask * dot(mask, upper), axis=0, keepdims=True).astype(jnp.int32)
        return dest, level_to, rank

    tab_ref[...] = jnp.zeros_like(tab_ref)
    _, level_to, rank = classify(depth)
    slots = iota((depths * LANES, own_blocks), 0)
    pick = (slots == level_to * LANES + rank).astype(f32)
    value = jnp.broadcast_to(lane, (ROWS, own_blocks)).astype(f32)
    got = dot(value, pick, ((1,), (1,))).astype(jnp.int32)
    for t in range(depths):
        tab_ref[t : t + 1, :] = got[0:1, t * LANES : (t + 1) * LANES]

    slots = iota((planes * P_TABLE, own_blocks), 0)
    before = jnp.zeros((ROWS, 1), f32)
    table = jnp.zeros((ROWS, planes * P_TABLE), f32)
    for level in range(depths):
        dest, level_to, rank = classify(level)
        here = level_to == depth
        plane_to = plane_of(dest, peers)
        mask = ((row8 == plane_to) & here).astype(f32)
        rank3 = jnp.sum(mask * (dot(mask, upper) + before), axis=0, keepdims=True)
        before = before + jnp.sum(mask, axis=1, keepdims=True)
        key = jnp.where(here, plane_to * P_TABLE + rank3.astype(jnp.int32), -1)
        pick = (slots == key).astype(f32)
        value = jnp.where(row8 == 0, rank, 1).astype(f32)
        got = dot(value, pick, ((1,), (1,)))
        table = table + got + float(level * Z_STRIDE) * got[1:2, :]
    table = table.astype(jnp.int32)
    table = jnp.clip(table, 0, depths * Z_STRIDE - 1)
    wide = planes * P_TABLE // LANES
    for t in range(wide):
        tab_ref[depths + t : depths + t + 1, :] = table[0:1, t * LANES : (t + 1) * LANES]

    part = part_ref[...]
    mine = iota((devices, LANES), 0) == d
    my_start = jnp.sum(jnp.where(mine, starts_i, 0), axis=0, keepdims=True)
    my_count = jnp.sum(jnp.where(mine, counts, 0), axis=0, keepdims=True)
    few = (iota((devices, own_blocks), 0) == part).astype(f32)
    rank = jnp.sum(few * dot(few, upper), axis=0, keepdims=True).astype(jnp.int32)
    pick = (source_rows == part).astype(f32)
    start8 = jnp.broadcast_to(my_start, (ROWS, LANES))
    begin = dot(start8.astype(f32), pick).astype(jnp.int32)[0:1]
    at = begin + rank
    part_plane = plane_of(part, peers)
    middle = (at % planes) ^ part_plane
    ids = iota((1, LANES), 1)
    residue = iota((ROWS, LANES), 0) ^ plane_of(ids, peers)
    in_use = ids < devices
    share = ((start8 + my_count + (shift - residue)) // planes) - (
        (start8 + (shift - residue)) // planes
    )
    share = jnp.where(in_use, share, 0)

    def order_of(p):
        return jnp.where(
            p < devices, depth_of(p, peers) * planes + plane_of(p, peers), LANES
        )

    ahead = (
        order_of(iota((LANES, LANES), 0)) < order_of(iota((LANES, LANES), 1))
    ).astype(f32)
    base = dot(share.astype(f32), ahead)
    base = dot(base, pick)
    base = jnp.sum(jnp.where(row8 == middle, base, 0.0), axis=0, keepdims=True)
    first = (begin + (shift - at % planes)) // planes
    final = middle * P_STRIDE + base.astype(jnp.int32) + at // planes - first
    final = jnp.clip(final, 0, planes * P_STRIDE - 1)
    row = depths + wide
    for t in range(own_blocks // LANES):
        tab_ref[row + t : row + t + 1, :] = final[:, t * LANES : (t + 1) * LANES]

    by_slab = (
        depth_of(iota((ROWS, devices), 1), peers) == iota((ROWS, devices), 0)
    ).astype(f32)
    rows = iota((LANES, LANES), 0)
    by_part = (
        (depth_of(rows, peers) == iota((LANES, LANES), 1)) & (rows < devices)
    ).astype(f32)
    far = ((iota((ROWS, LANES), 0) ^ iota((ROWS, LANES), 1)) & 2) != 0
    level_most = jnp.zeros((ROWS, LANES), f32)
    plane_most = jnp.zeros((devices, 1), f32)
    for k in range(planes):
        left = shift - (k ^ plane_of(ids, peers))
        some = (starts_i + counts + left) // planes - (starts_i + left) // planes
        some = jnp.where(in_use, some, 0).astype(f32)
        plane_most = jnp.maximum(plane_most, jnp.sum(some, axis=1, keepdims=True))
        level_most = jnp.maximum(level_most, dot(dot(by_slab, some), by_part))
    used = jnp.max(jnp.where(far, level_most, 0.0)).astype(jnp.int32)
    most = jnp.max(level_most).astype(jnp.int32)
    final_most = jnp.max(plane_most).astype(jnp.int32)
    tier = jnp.int32(len(TIERS))
    for t in range(len(TIERS) - 1, -1, -1):
        room, room3 = TIERS[t]
        fits = (used <= room) & (final_most <= room3) & (most <= Z_NEAR)
        tier = jnp.where(fits, t, tier)
    tier_ref[0] = tier


def make_tables(counts, part, devices, peers, own_blocks):
    return pl.pallas_call(
        functools.partial(table_kernel, devices, peers, own_blocks),
        out_shape=(
            jax.ShapeDtypeStruct((2 * ROWS, LANES), jnp.int32),
            jax.ShapeDtypeStruct((1,), jnp.int32),
        ),
        in_specs=[
            pl.BlockSpec(memory_space=pltpu.VMEM),
            pl.BlockSpec(memory_space=pltpu.VMEM),
        ],
        out_specs=(
            pl.BlockSpec(memory_space=pltpu.VMEM),
            pl.BlockSpec(memory_space=pltpu.SMEM),
        ),
    )(counts, part)


def exchange_kernel(peers, own_blocks, tiles, rooms, tables, params, states, out, out_row, *refs):
    d = my_index(peers)
    plane = plane_of(d, peers)
    depth = depth_of(d, peers)
    planes = ROWS
    depths = peers // 2
    per = own_blocks // planes
    chunks = tiles + 1
    unroll = 8
    own, own_row = refs[0:2]
    at = 2
    groups = []
    for _ in range(6):
        groups.append(refs[at : at + chunks])
        at += chunks
    landed1, packed2, landed2, packed3, landed3, ready = groups
    send_sem, recv_sem, out_sem = refs[at:]
    room2 = (None, Z_NEAR, rooms[0], rooms[0])
    room3 = rooms[1]
    wide = planes * P_TABLE // LANES

    def device(to_plane, to_depth):
        return (to_plane // 2, to_depth * 2 + to_plane % 2)

    barrier = pltpu.get_barrier_semaphore()
    partners = [device(plane ^ m, depth) for m in range(1, planes)]
    partners += [device(plane, depth ^ m) for m in range(1, depths)]
    for to in partners:
        pl.semaphore_signal(barrier, inc=1, device_id=to, device_id_type=MESH_ID)

    def advance_block(i, u):
        cols = pl.ds(pl.multiple_of((i * planes + u) * LANES, LANES), LANES)
        top = states[0:ROWS, cols]
        voltage = top[0:1, :]
        spread = jnp.broadcast_to(voltage, (ROWS, LANES))
        slow = -(1.0 + jax.nn.sigmoid(spread))

        def gates(vals, base, count):
            half, steep, rate, cond, rev = (
                params[k, base : base + count, :] for k in range(5)
            )
            v = spread[0:count]
            steady = jax.nn.sigmoid((v - half) * steep)
            damping = jnp.exp(rate * slow[0:count])
            new = steady + (vals - steady) * damping
            return new, cond * new * (v - rev)

        def put(c, value):
            if u == 0:
                landed1[c][plane * per + i] = value
            else:
                own[c, u - 1, i] = value

        total = jnp.zeros((ROWS, LANES), jnp.float32)
        for t in range(1, tiles):
            new, term = gates(states[t * ROWS : (t + 1) * ROWS, cols], t * ROWS, ROWS)
            put(t, new)
            total = total + term
        last = tiles * ROWS
        new_row, term_row = gates(states[last : last + 1, cols], last, 1)
        if u == 0:
            landed1[tiles][pl.ds(plane * per + i, 1), :] = new_row
        else:
            own_row[u - 1, pl.ds(i, 1), :] = new_row
        new, term = gates(top, 0, ROWS)
        total = total + term
        current = jnp.sum(total, axis=0, keepdims=True) + term_row
        moved = voltage - time_step * current
        first = lax.broadcasted_iota(jnp.int32, (ROWS, LANES), 0) == 0
        put(0, jnp.where(first, jnp.broadcast_to(moved, (ROWS, LANES)), new))

    def advance_loop(i, _):
        for u in range(planes):
            advance_block(i, u)
        return 0

    lax.fori_loop(0, per, advance_loop, 0)
    pl.semaphore_wait(barrier, len(partners))

    copies = {}

    def send(c, phase, m, src, dst, to):
        copy = pltpu.make_async_remote_copy(
            src_ref=src,
            dst_ref=dst,
            send_sem=send_sem.at[c, phase, m],
            recv_sem=recv_sem.at[c, phase, m],
            device_id=to,
            device_id_type=MESH_ID,
        )
        copy.start()
        copies[(c, phase, m)] = copy

    def gather(c, count, table_row, table_col, src, put, first):
        def body(i, _):
            for u in range(unroll):
                k = i * unroll + u
                where = tables[table_row, table_col + k]
                if c < tiles:
                    put[first + k] = src[where]
                else:
                    put[pl.ds(first + k, 1), :] = src[pl.ds(where, 1), :]
            return 0

        lax.fori_loop(0, count // unroll, body, 0)

    def phase1(c):
        source = own.at[c] if c < tiles else own_row
        for m in range(1, planes):
            send(
                c, 0, m, source.at[m - 1], landed1[c].at[pl.ds(plane * per, per)],
                device(plane ^ m, depth),
            )

    def phase2(c):
        for m in range(1, planes):
            copies[(c, 0, m)].wait_recv()
        for m in (2, 3, 1):
            gather(c, room2[m], depth ^ m, 0, landed1[c], packed2[c].at[m - 1], 0)
            send(
                c, 1, m, packed2[c].at[m - 1, pl.ds(0, room2[m])],
                landed2[c].at[pl.ds(depth * Z_STRIDE, room2[m])],
                device(plane, depth ^ m),
            )
        gather(c, Z_NEAR, depth, 0, landed1[c], landed2[c], depth * Z_STRIDE)

    def phase3(c):
        for m in range(1, depths):
            copies[(c, 1, m)].wait_recv()
        for m in (6, 7, 4, 5, 1, 3, 2):
            to = plane ^ m
            gather(
                c, room3, depths + to // 2, (to % 2) * P_TABLE,
                landed2[c], packed3[c].at[m - 1], 0,
            )
            send(
                c, 2, m, packed3[c].at[m - 1, pl.ds(0, room3)],
                landed3[c].at[pl.ds(plane * P_STRIDE, room3)],
                device(to, depth),
            )
        gather(
            c, room3, depths + plane // 2, (plane % 2) * P_TABLE,
            landed2[c], landed3[c], plane * P_STRIDE,
        )

    outs = []

    def finish(c):
        for m in range(1, planes):
            copies[(c, 2, m)].wait_recv()
        for t in range(own_blocks // LANES):
            gather(c, LANES, depths + wide + t, 0, landed3[c], ready[c], t * LANES)
        copy = pltpu.make_async_copy(
            ready[c], out.at[c] if c < tiles else out_row, out_sem.at[c]
        )
        copy.start()
        outs.append(copy)

    for phase, c in EVENTS:
        (phase1, phase2, phase3, finish)[phase](c)
    for copy in outs:
        copy.wait()
    for copy in copies.values():
        copy.wait_send()


EVENTS = (
    (0, 0), (0, 1), (0, 2), (0, 3), (1, 0), (1, 1), (1, 2), (2, 0), (0, 4), (0, 5), (1, 3),
    (2, 1), (1, 4), (1, 5), (3, 0), (2, 2), (3, 1), (2, 3), (3, 2), (2, 4), (2, 5), (3, 3),
    (3, 4), (3, 5),
)


def exchange(tables, params, states, peers, own_blocks, rooms):
    tiles = states.shape[0] // ROWS
    planes = ROWS
    depths = peers // 2
    per = own_blocks // planes
    f32 = jnp.float32

    def buffers(*lead):
        kinds = [pltpu.VMEM(lead + (ROWS, LANES), f32) for _ in range(tiles)]
        return kinds + [pltpu.VMEM(lead + (LANES,), f32)]

    return pl.pallas_call(
        functools.partial(exchange_kernel, peers, own_blocks, tiles, rooms),
        out_shape=(
            jax.ShapeDtypeStruct((tiles, own_blocks, ROWS, LANES), f32),
            jax.ShapeDtypeStruct((own_blocks, LANES), f32),
        ),
        in_specs=[
            pl.BlockSpec(memory_space=pltpu.SMEM),
            pl.BlockSpec(memory_space=pltpu.VMEM),
            pl.BlockSpec(memory_space=pltpu.VMEM),
        ],
        out_specs=(
            pl.BlockSpec(memory_space=pl.ANY),
            pl.BlockSpec(memory_space=pl.ANY),
        ),
        scratch_shapes=[
            pltpu.VMEM((tiles, planes - 1, per, ROWS, LANES), f32),
            pltpu.VMEM((planes - 1, per, LANES), f32),
            *buffers(own_blocks),
            *buffers(depths - 1, Z_STRIDE),
            *buffers(depths * Z_STRIDE),
            *buffers(planes - 1, P_STRIDE),
            *buffers(planes * P_STRIDE),
            *buffers(own_blocks),
            pltpu.SemaphoreType.DMA((tiles + 1, 3, planes)),
            pltpu.SemaphoreType.DMA((tiles + 1, 3, planes)),
            pltpu.SemaphoreType.DMA((tiles + 1,)),
        ],
        compiler_params=pltpu.CompilerParams(
            collective_id=1 + TIERS.index(rooms),
            has_side_effects=True,
            vmem_limit_bytes=VMEM_LIMIT,
        ),
    )(tables, params, states)


def place_kernel(tiles, blocks, got, got_row, perm, out):
    for group in range(blocks // ROWS):
        rows = slice(group * ROWS, (group + 1) * ROWS)
        turned = jnp.take_along_axis(
            got_row[rows, :], perm[rows, :], axis=1, mode="promise_in_bounds"
        )
        for u in range(ROWS):
            b = group * ROWS + u
            cols = slice(b * LANES, (b + 1) * LANES)
            where = jnp.broadcast_to(perm[b : b + 1, :], (ROWS, LANES))
            for t in range(tiles):
                out[t * ROWS : (t + 1) * ROWS, cols] = jnp.take_along_axis(
                    got[t, b], where, axis=1, mode="promise_in_bounds"
                )
            out[tiles * ROWS : tiles * ROWS + 1, cols] = turned[u : u + 1, :]


def place(got, got_row, perm, width, own_blocks):
    tiles = got.shape[0]
    step = 32
    return pl.pallas_call(
        functools.partial(place_kernel, tiles, step),
        grid=(own_blocks // step,),
        out_shape=jax.ShapeDtypeStruct((width, own_blocks * LANES), jnp.float32),
        in_specs=[
            pl.BlockSpec((tiles, step, ROWS, LANES), lambda i: (0, i, 0, 0)),
            pl.BlockSpec((step, LANES), lambda i: (i, 0)),
            pl.BlockSpec((step, LANES), lambda i: (i, 0)),
        ],
        out_specs=pl.BlockSpec((width, step * LANES), lambda i: (0, i)),
    )(got, got_row, perm)


def advance(state_rows, half_volt, steepness, gate_rate, conductance, reversal):
    voltage = state_rows[0:1]
    gate_vals = state_rows[1:]
    steady = jax.nn.sigmoid((voltage - half_volt[:, None]) * steepness[:, None])
    damping = jnp.exp(-gate_rate[:, None] * (1.0 + jax.nn.sigmoid(voltage)))
    gate_vals = steady + (gate_vals - steady) * damping
    current = jnp.sum(
        conductance[:, None] * gate_vals * (voltage - reversal[:, None]), axis=0, keepdims=True
    )
    voltage = voltage - time_step * current
    return jnp.concatenate([voltage, gate_vals], axis=0)


def general(counts_all, devices, states, block_part, tile_perm, *gate_params):
    d = lax.axis_index(("group", "peer"))
    local_blocks = block_part.shape[0]
    tile_width = tile_perm.shape[1]
    width = states.shape[0]
    capacity = 2 * local_blocks // devices
    partitions = jnp.arange(devices, dtype=jnp.int32)
    onehot = (block_part[:, None] == partitions[None, :]).astype(jnp.int32)
    before = (partitions < d).astype(jnp.int32)
    earlier = jnp.sum(counts_all * before[:, None], axis=0, dtype=jnp.int32)
    rank_in = jnp.sum(
        (jnp.cumsum(onehot, axis=0, dtype=jnp.int32) - onehot) * onehot, axis=1, dtype=jnp.int32
    )
    local_index = jnp.sum(onehot * earlier[None, :], axis=1, dtype=jnp.int32) + rank_in
    slot_index = block_part * capacity + rank_in
    requests = jnp.full((devices * capacity,), -1, jnp.int32).at[slot_index].set(local_index)
    requests = requests.reshape(devices, capacity)
    advanced = advance(states, *gate_params)
    advanced = advanced.reshape(width, local_blocks, tile_width)
    wanted = lax.all_to_all(requests, ("group", "peer"), split_axis=0, concat_axis=0, tiled=True)
    picked = jnp.maximum(wanted, 0).reshape(-1)
    served = jnp.take(advanced, picked, axis=1)
    arrived = lax.all_to_all(
        served.reshape(width, wanted.shape[0], wanted.shape[1], tile_width),
        ("group", "peer"), split_axis=1, concat_axis=1, tiled=True,
    )
    flat_cols = (slot_index[:, None] * tile_width + tile_perm).reshape(-1)
    return jnp.take(arrived.reshape(width, devices * capacity * tile_width), flat_cols, axis=1)


def on_device(devices, peers, states, block_part, tile_perm, *gate_params):
    own_blocks = block_part.shape[0]
    width = states.shape[0]
    partitions = jnp.arange(LANES, dtype=jnp.int32)
    counts = jnp.sum(
        (block_part[:, None] == partitions[None, :]).astype(jnp.int32), axis=0, dtype=jnp.int32
    )
    if (devices, peers) != (4 * ROWS, ROWS) or width % ROWS != 1:
        gathered = lax.all_gather(counts[:devices], ("group", "peer"))
        return general(gathered, devices, states, block_part, tile_perm, *gate_params)
    gathered = gather_counts(counts.reshape(1, 1, LANES), devices, peers)
    tables, tier = make_tables(
        gathered, block_part.reshape(1, own_blocks), devices, peers, own_blocks
    )
    padded = jnp.stack([jnp.pad(p, (1, 0)) for p in gate_params])
    params = jnp.broadcast_to(padded[:, :, None], padded.shape + (LANES,))

    def fast(rooms):
        got, got_row = exchange(tables, params, states, peers, own_blocks, rooms)
        return place(got, got_row, tile_perm, width, own_blocks)

    def slow():
        matrix = gathered[:, 0, :devices]
        return general(matrix, devices, states, block_part, tile_perm, *gate_params)

    choices = [functools.partial(fast, rooms) for rooms in TIERS] + [slow]
    return lax.switch(tier[0], choices)


def solution(mesh):
    both = P(("group", "peer"))
    return jax.shard_map(
        functools.partial(on_device, mesh.devices.size, mesh.shape["peer"]),
        mesh=mesh,
        in_specs=(P(None, ("group", "peer")), both, P(("group", "peer"), None)) + (P(),) * 5,
        out_specs=P(None, ("group", "peer")),
        check_vma=False,
    )
```

```python
import functools
import jax
import jax.numpy as jnp
import numpy as np
from jax import lax
from jax.experimental import pallas as pl
from jax.experimental.pallas import tpu as pltpu
from jax.sharding import PartitionSpec as P

time_step = 0.25
LANES = 128
ROWS = 8
MESH_ID = pl.DeviceIdType.MESH
VMEM_LIMIT = 67043328
Z_STRIDE = 88
Z_NEAR = 88
P_STRIDE = 48
P_TABLE = 64
PIECES = 4
TIERS = ((72, 40), (80, 40), (88, 48))


def my_index(peers):
    return lax.axis_index("group") * peers + lax.axis_index("peer")


def plane_of(d, peers):
    return (d // peers) * 2 + d % 2


def depth_of(d, peers):
    return (d % peers) // 2


def dot(a, b, contract=((1,), (0,))):
    return lax.dot_general(
        a, b, (contract, ((), ())), preferred_element_type=jnp.float32
    )


def iota(shape, axis):
    return lax.broadcasted_iota(jnp.int32, shape, axis)


def fill_tables(devices, peers, own_blocks, c_ref, part_ref, tab_ref, tier_ref):
    d = my_index(peers)
    plane = plane_of(d, peers)
    depth = depth_of(d, peers)
    planes = ROWS
    depths = peers // 2
    per = own_blocks // planes
    f32 = jnp.float32
    shift = ROWS - 1
    counts = c_ref[...].reshape(devices, LANES)
    lower = (iota((devices, devices), 1) < iota((devices, devices), 0)).astype(f32)
    starts = dot(lower, counts.astype(f32))
    starts_i = starts.astype(jnp.int32)
    upper = (
        iota((own_blocks, own_blocks), 0) < iota((own_blocks, own_blocks), 1)
    ).astype(f32)
    lane = iota((1, own_blocks), 1)
    lane_plane = lane // per
    stored = (lane % per) * planes + (plane ^ lane_plane)
    source_rows = iota((LANES, own_blocks), 0)
    row8 = iota((ROWS, own_blocks), 0)

    def classify(level):
        source = (lane_plane // 2) * peers + level * 2 + lane_plane % 2
        pick = (source_rows == source).astype(f32)
        begin = dot(starts, pick).astype(jnp.int32)
        dest = jnp.sum((begin <= stored).astype(jnp.int32), axis=0, keepdims=True) - 1
        level_to = depth_of(dest, peers)
        mask = (row8 == level_to).astype(f32)
        rank = jnp.sum(mask * dot(mask, upper), axis=0, keepdims=True).astype(jnp.int32)
        return dest, level_to, rank

    tab_ref[...] = jnp.zeros_like(tab_ref)
    _, level_to, rank = classify(depth)
    slots = iota((depths * LANES, own_blocks), 0)
    pick = (slots == level_to * LANES + rank).astype(f32)
    value = jnp.broadcast_to(lane, (ROWS, own_blocks)).astype(f32)
    got = dot(value, pick, ((1,), (1,))).astype(jnp.int32)
    for t in range(depths):
        tab_ref[t : t + 1, :] = got[0:1, t * LANES : (t + 1) * LANES]

    slots = iota((planes * P_TABLE, own_blocks), 0)
    before = jnp.zeros((ROWS, 1), f32)
    table = jnp.zeros((ROWS, planes * P_TABLE), f32)
    for level in range(depths):
        dest, level_to, rank = classify(level)
        here = level_to == depth
        plane_to = plane_of(dest, peers)
        mask = ((row8 == plane_to) & here).astype(f32)
        rank3 = jnp.sum(mask * (dot(mask, upper) + before), axis=0, keepdims=True)
        before = before + jnp.sum(mask, axis=1, keepdims=True)
        key = jnp.where(here, plane_to * P_TABLE + rank3.astype(jnp.int32), -1)
        pick = (slots == key).astype(f32)
        value = jnp.where(row8 == 0, rank, 1).astype(f32)
        got = dot(value, pick, ((1,), (1,)))
        table = table + got + float(level * Z_STRIDE) * got[1:2, :]
    table = table.astype(jnp.int32)
    table = jnp.clip(table, 0, depths * Z_STRIDE - 1)
    wide = planes * P_TABLE // LANES
    for t in range(wide):
        tab_ref[depths + t : depths + t + 1, :] = table[0:1, t * LANES : (t + 1) * LANES]

    part = part_ref[...]
    mine = iota((devices, LANES), 0) == d
    my_start = jnp.sum(jnp.where(mine, starts_i, 0), axis=0, keepdims=True)
    my_count = jnp.sum(jnp.where(mine, counts, 0), axis=0, keepdims=True)
    few = (iota((devices, own_blocks), 0) == part).astype(f32)
    rank = jnp.sum(few * dot(few, upper), axis=0, keepdims=True).astype(jnp.int32)
    pick = (source_rows == part).astype(f32)
    start8 = jnp.broadcast_to(my_start, (ROWS, LANES))
    begin = dot(start8.astype(f32), pick).astype(jnp.int32)[0:1]
    at = begin + rank
    part_plane = plane_of(part, peers)
    middle = (at % planes) ^ part_plane
    ids = iota((1, LANES), 1)
    residue = iota((ROWS, LANES), 0) ^ plane_of(ids, peers)
    in_use = ids < devices
    share = ((start8 + my_count + (shift - residue)) // planes) - (
        (start8 + (shift - residue)) // planes
    )
    share = jnp.where(in_use, share, 0)

    def order_of(p):
        return jnp.where(
            p < devices, depth_of(p, peers) * planes + plane_of(p, peers), LANES
        )

    ahead = (
        order_of(iota((LANES, LANES), 0)) < order_of(iota((LANES, LANES), 1))
    ).astype(f32)
    base = dot(share.astype(f32), ahead)
    base = dot(base, pick)
    base = jnp.sum(jnp.where(row8 == middle, base, 0.0), axis=0, keepdims=True)
    first = (begin + (shift - at % planes)) // planes
    final = middle * P_STRIDE + base.astype(jnp.int32) + at // planes - first
    final = jnp.clip(final, 0, planes * P_STRIDE - 1)
    row = depths + wide
    for t in range(own_blocks // LANES):
        tab_ref[row + t : row + t + 1, :] = final[:, t * LANES : (t + 1) * LANES]

    by_slab = (
        depth_of(iota((ROWS, devices), 1), peers) == iota((ROWS, devices), 0)
    ).astype(f32)
    rows = iota((LANES, LANES), 0)
    by_part = (
        (depth_of(rows, peers) == iota((LANES, LANES), 1)) & (rows < devices)
    ).astype(f32)
    far = ((iota((ROWS, LANES), 0) ^ iota((ROWS, LANES), 1)) & 2) != 0
    level_most = jnp.zeros((ROWS, LANES), f32)
    plane_most = jnp.zeros((devices, 1), f32)
    for k in range(planes):
        left = shift - (k ^ plane_of(ids, peers))
        some = (starts_i + counts + left) // planes - (starts_i + left) // planes
        some = jnp.where(in_use, some, 0).astype(f32)
        plane_most = jnp.maximum(plane_most, jnp.sum(some, axis=1, keepdims=True))
        level_most = jnp.maximum(level_most, dot(dot(by_slab, some), by_part))
    used = jnp.max(jnp.where(far, level_most, 0.0)).astype(jnp.int32)
    most = jnp.max(level_most).astype(jnp.int32)
    final_most = jnp.max(plane_most).astype(jnp.int32)
    tier = jnp.int32(len(TIERS))
    for t in range(len(TIERS) - 1, -1, -1):
        room, room3 = TIERS[t]
        fits = (used <= room) & (final_most <= room3) & (most <= Z_NEAR)
        tier = jnp.where(fits, t, tier)
    tier_ref[0] = tier


def opening_kernel(
    devices, peers, own_blocks, tiles,
    part_ref, half_ref, steep_ref, rate_ref, cond_ref, rev_ref, states_ref,
    tab_ref, tier_ref, counts_out, own_out, row_out, first_out,
    states, params, own, own_row, landed, tally, counts,
    load_sem, count_send, count_recv, send_sem, recv_sem, out_sem,
):
    d = my_index(peers)
    plane = plane_of(d, peers)
    depth = depth_of(d, peers)
    planes = ROWS
    per = own_blocks // planes
    step = per // PIECES
    width = step * planes * LANES

    loads = []
    for q in range(PIECES):
        cols = pl.ds(q * width, width)
        copy = pltpu.make_async_copy(
            states_ref.at[:, cols], states.at[:, cols], load_sem.at[q]
        )
        copy.start()
        loads.append(copy)

    barrier = pltpu.get_barrier_semaphore()
    for k in range(1, devices):
        to = (d + k) % devices
        pl.semaphore_signal(
            barrier, inc=1, device_id=(to // peers, to % peers), device_id_type=MESH_ID
        )

    match = (iota((LANES, own_blocks), 0) == part_ref[...]).astype(jnp.float32)
    ones = jnp.ones((ROWS, own_blocks), jnp.float32)
    tally[...] = dot(ones, match, ((1,), (1,)))[0:1].astype(jnp.int32)
    counts[d] = tally[...]
    gates_all = half_ref.shape[1]
    for k, ref in enumerate((half_ref, steep_ref, rate_ref, cond_ref, rev_ref)):
        for base in range(0, tiles * ROWS + ROWS, ROWS):
            shape = (ROWS, gates_all)
            chosen = iota(shape, 1) == iota(shape, 0) + (base - 1)
            column = jnp.sum(jnp.where(chosen, ref[...], 0.0), axis=1, keepdims=True)
            params[k, base : base + ROWS, :] = jnp.broadcast_to(column, (ROWS, LANES))

    def advance_block(i, u):
        cols = pl.ds(pl.multiple_of((i * planes + u) * LANES, LANES), LANES)
        top = states[0:ROWS, cols]
        voltage = top[0:1, :]
        spread = jnp.broadcast_to(voltage, (ROWS, LANES))
        slow = -(1.0 + jax.nn.sigmoid(spread))

        def gates(vals, base, count):
            half, steep, rate, cond, rev = (
                params[k, base : base + count, :] for k in range(5)
            )
            v = spread[0:count]
            steady = jax.nn.sigmoid((v - half) * steep)
            damping = jnp.exp(rate * slow[0:count])
            new = steady + (vals - steady) * damping
            return new, cond * new * (v - rev)

        total = jnp.zeros((ROWS, LANES), jnp.float32)
        for t in range(1, tiles):
            new, term = gates(states[t * ROWS : (t + 1) * ROWS, cols], t * ROWS, ROWS)
            own[t - 1, u, i] = new
            total = total + term
        last = tiles * ROWS
        new_row, term_row = gates(states[last : last + 1, cols], last, 1)
        own_row[u, pl.ds(i, 1), :] = new_row
        new, term = gates(top, 0, ROWS)
        total = total + term
        current = jnp.sum(total, axis=0, keepdims=True) + term_row
        moved = voltage - time_step * current
        first = lax.broadcasted_iota(jnp.int32, (ROWS, LANES), 0) == 0
        value = jnp.where(first, jnp.broadcast_to(moved, (ROWS, LANES)), new)
        if u == 0:
            landed[plane * per + i] = value
        else:
            own[tiles - 1, u, i] = value

    def advance_loop(i, _):
        for u in range(planes):
            advance_block(i, u)
        return 0

    sends = []
    outs = []
    count_copies = []
    for q in range(PIECES):
        loads[q].wait()
        lax.fori_loop(q * step, (q + 1) * step, advance_loop, 0)
        if q == 0:
            pl.semaphore_wait(barrier, devices - 1)
            for k in range(1, devices):
                to = (d + k) % devices
                copy = pltpu.make_async_remote_copy(
                    src_ref=tally, dst_ref=counts.at[d],
                    send_sem=count_send.at[k], recv_sem=count_recv.at[k],
                    device_id=(to // peers, to % peers), device_id_type=MESH_ID,
                )
                copy.start()
                count_copies.append(copy)
        for m in (6, 7, 4, 5, 1, 3, 2):
            to = plane ^ m
            copy = pltpu.make_async_remote_copy(
                src_ref=own.at[tiles - 1, m, pl.ds(q * step, step)],
                dst_ref=landed.at[pl.ds(plane * per + q * step, step)],
                send_sem=send_sem.at[q, m], recv_sem=recv_sem.at[q, m],
                device_id=(to // 2, depth * 2 + to % 2), device_id_type=MESH_ID,
            )
            copy.start()
            sends.append(copy)
        some = pl.ds(q * step, step)
        copy = pltpu.make_async_copy(
            own.at[pl.ds(0, tiles - 1), :, some], own_out.at[:, :, some], out_sem.at[q, 0]
        )
        copy.start()
        outs.append(copy)
        copy = pltpu.make_async_copy(
            own_row.at[:, some], row_out.at[:, some], out_sem.at[q, 1]
        )
        copy.start()
        outs.append(copy)
    for copy in count_copies:
        copy.wait_recv()
    counts_out[...] = counts[...]
    fill_tables(devices, peers, own_blocks, counts, part_ref, tab_ref, tier_ref)
    for copy in sends:
        copy.wait_recv()
    copy = pltpu.make_async_copy(landed, first_out, out_sem.at[PIECES, 0])
    copy.start()
    outs.append(copy)
    for copy in count_copies + sends:
        copy.wait_send()
    for copy in outs:
        copy.wait()


def opening(part, gate_params, states, devices, peers):
    own_blocks = part.shape[1]
    tiles = states.shape[0] // ROWS
    planes = ROWS
    per = own_blocks // planes
    f32 = jnp.float32
    vmem = pl.BlockSpec(memory_space=pltpu.VMEM)
    anywhere = pl.BlockSpec(memory_space=pl.ANY)
    return pl.pallas_call(
        functools.partial(opening_kernel, devices, peers, own_blocks, tiles),
        out_shape=(
            jax.ShapeDtypeStruct((2 * ROWS, LANES), jnp.int32),
            jax.ShapeDtypeStruct((1,), jnp.int32),
            jax.ShapeDtypeStruct((devices, 1, LANES), jnp.int32),
            jax.ShapeDtypeStruct((tiles - 1, planes, per, ROWS, LANES), f32),
            jax.ShapeDtypeStruct((planes, per, LANES), f32),
            jax.ShapeDtypeStruct((own_blocks, ROWS, LANES), f32),
        ),
        in_specs=[vmem] * 6 + [anywhere],
        out_specs=(
            vmem, pl.BlockSpec(memory_space=pltpu.SMEM), vmem, anywhere, anywhere, anywhere,
        ),
        scratch_shapes=[
            pltpu.VMEM(states.shape, f32),
            pltpu.VMEM((5, (tiles + 1) * ROWS, LANES), f32),
            pltpu.VMEM((tiles, planes, per, ROWS, LANES), f32),
            pltpu.VMEM((planes, per, LANES), f32),
            pltpu.VMEM((own_blocks, ROWS, LANES), f32),
            pltpu.VMEM((1, LANES), jnp.int32),
            pltpu.VMEM((devices, 1, LANES), jnp.int32),
            pltpu.SemaphoreType.DMA((PIECES,)),
            pltpu.SemaphoreType.DMA((devices,)),
            pltpu.SemaphoreType.DMA((devices,)),
            pltpu.SemaphoreType.DMA((PIECES, planes)),
            pltpu.SemaphoreType.DMA((PIECES, planes)),
            pltpu.SemaphoreType.DMA((PIECES + 1, 2)),
        ],
        compiler_params=pltpu.CompilerParams(
            collective_id=0, has_side_effects=True, vmem_limit_bytes=VMEM_LIMIT
        ),
    )(part, *gate_params, states)


def exchange_kernel(peers, own_blocks, tiles, rooms, tables, own, own_row, ahead, out, out_row, *refs):
    d = my_index(peers)
    plane = plane_of(d, peers)
    depth = depth_of(d, peers)
    planes = ROWS
    depths = peers // 2
    per = own_blocks // planes
    chunks = tiles + 1
    unroll = 8
    at = 0
    groups = []
    for _ in range(6):
        groups.append(refs[at : at + chunks])
        at += chunks
    landed1, packed2, landed2, packed3, landed3, ready = groups
    send_sem, recv_sem, out_sem, in_sem = refs[at:]
    room2 = (None, Z_NEAR, rooms[0], rooms[0])
    room3 = rooms[1]
    wide = planes * P_TABLE // LANES

    def device(to_plane, to_depth):
        return (to_plane // 2, to_depth * 2 + to_plane % 2)

    barrier = pltpu.get_barrier_semaphore()
    partners = [device(plane ^ m, depth) for m in range(1, planes)]
    partners += [device(plane, depth ^ m) for m in range(1, depths)]
    for to in partners:
        pl.semaphore_signal(barrier, inc=1, device_id=to, device_id_type=MESH_ID)

    loads = [pltpu.make_async_copy(ahead, landed1[0], in_sem.at[0])]
    for c in range(1, chunks):
        source = own.at[c - 1, 0] if c < tiles else own_row.at[0]
        loads.append(
            pltpu.make_async_copy(
                source, landed1[c].at[pl.ds(plane * per, per)], in_sem.at[c]
            )
        )
    for copy in loads:
        copy.start()
    pl.semaphore_wait(barrier, len(partners))

    copies = {}

    def send(c, phase, m, src, dst, to):
        copy = pltpu.make_async_remote_copy(
            src_ref=src,
            dst_ref=dst,
            send_sem=send_sem.at[c, phase, m],
            recv_sem=recv_sem.at[c, phase, m],
            device_id=to,
            device_id_type=MESH_ID,
        )
        copy.start()
        copies[(c, phase, m)] = copy

    def gather(c, count, table_row, table_col, src, put, first):
        def body(i, _):
            for u in range(unroll):
                k = i * unroll + u
                where = tables[table_row, table_col + k]
                if c < tiles:
                    put[first + k] = src[where]
                else:
                    put[pl.ds(first + k, 1), :] = src[pl.ds(where, 1), :]
            return 0

        lax.fori_loop(0, count // unroll, body, 0)

    def phase1(c):
        source = own.at[c - 1] if c < tiles else own_row
        for m in (6, 7, 4, 5, 1, 3, 2):
            send(
                c, 0, m, source.at[m], landed1[c].at[pl.ds(plane * per, per)],
                device(plane ^ m, depth),
            )

    def phase2(c):
        loads[c].wait()
        for m in range(1, planes if c else 1):
            copies[(c, 0, m)].wait_recv()
        for m in (2, 3, 1):
            gather(c, room2[m], depth ^ m, 0, landed1[c], packed2[c].at[m - 1], 0)
            send(
                c, 1, m, packed2[c].at[m - 1, pl.ds(0, room2[m])],
                landed2[c].at[pl.ds(depth * Z_STRIDE, room2[m])],
                device(plane, depth ^ m),
            )
        gather(c, Z_NEAR, depth, 0, landed1[c], landed2[c], depth * Z_STRIDE)

    def phase3(c):
        for m in range(1, depths):
            copies[(c, 1, m)].wait_recv()
        for m in (6, 7, 4, 5, 1, 3, 2):
            to = plane ^ m
            gather(
                c, room3, depths + to // 2, (to % 2) * P_TABLE,
                landed2[c], packed3[c].at[m - 1], 0,
            )
            send(
                c, 2, m, packed3[c].at[m - 1, pl.ds(0, room3)],
                landed3[c].at[pl.ds(plane * P_STRIDE, room3)],
                device(to, depth),
            )
        gather(
            c, room3, depths + plane // 2, (plane % 2) * P_TABLE,
            landed2[c], landed3[c], plane * P_STRIDE,
        )

    outs = []

    def finish(c):
        for m in range(1, planes):
            copies[(c, 2, m)].wait_recv()
        for t in range(own_blocks // LANES):
            gather(c, LANES, depths + wide + t, 0, landed3[c], ready[c], t * LANES)
        copy = pltpu.make_async_copy(
            ready[c], out.at[c] if c < tiles else out_row, out_sem.at[c]
        )
        copy.start()
        outs.append(copy)

    for phase, c in EVENTS:
        (phase1, phase2, phase3, finish)[phase](c)
    for copy in outs:
        copy.wait()
    for copy in copies.values():
        copy.wait_send()


EVENTS = (
    (0, 1), (1, 0), (0, 2), (0, 3), (1, 1), (1, 2), (2, 0), (0, 4), (0, 5), (1, 3),
    (2, 1), (1, 4), (1, 5), (3, 0), (2, 2), (3, 1), (2, 3), (3, 2), (2, 4), (2, 5), (3, 3),
    (3, 4), (3, 5),
)


def exchange(tables, own, own_row, ahead, peers, own_blocks, rooms):
    tiles = own.shape[0] + 1
    planes = ROWS
    depths = peers // 2
    per = own_blocks // planes
    f32 = jnp.float32

    def buffers(*lead):
        kinds = [pltpu.VMEM(lead + (ROWS, LANES), f32) for _ in range(tiles)]
        return kinds + [pltpu.VMEM(lead + (LANES,), f32)]

    return pl.pallas_call(
        functools.partial(exchange_kernel, peers, own_blocks, tiles, rooms),
        out_shape=(
            jax.ShapeDtypeStruct((tiles, own_blocks, ROWS, LANES), f32),
            jax.ShapeDtypeStruct((own_blocks, LANES), f32),
        ),
        in_specs=[
            pl.BlockSpec(memory_space=pltpu.SMEM),
            pl.BlockSpec(memory_space=pl.ANY),
            pl.BlockSpec(memory_space=pl.ANY),
            pl.BlockSpec(memory_space=pl.ANY),
        ],
        out_specs=(
            pl.BlockSpec(memory_space=pl.ANY),
            pl.BlockSpec(memory_space=pl.ANY),
        ),
        scratch_shapes=[
            *buffers(own_blocks),
            *buffers(depths - 1, Z_STRIDE),
            *buffers(depths * Z_STRIDE),
            *buffers(planes - 1, P_STRIDE),
            *buffers(planes * P_STRIDE),
            *buffers(own_blocks),
            pltpu.SemaphoreType.DMA((tiles + 1, 3, planes)),
            pltpu.SemaphoreType.DMA((tiles + 1, 3, planes)),
            pltpu.SemaphoreType.DMA((tiles + 1,)),
            pltpu.SemaphoreType.DMA((tiles + 1,)),
        ],
        compiler_params=pltpu.CompilerParams(
            collective_id=1 + TIERS.index(rooms),
            has_side_effects=True,
            vmem_limit_bytes=VMEM_LIMIT,
        ),
    )(tables, own, own_row, ahead)


def place_kernel(tiles, blocks, got, got_row, perm, out):
    for group in range(blocks // ROWS):
        rows = slice(group * ROWS, (group + 1) * ROWS)
        turned = jnp.take_along_axis(
            got_row[rows, :], perm[rows, :], axis=1, mode="promise_in_bounds"
        )
        for u in range(ROWS):
            b = group * ROWS + u
            cols = slice(b * LANES, (b + 1) * LANES)
            where = jnp.broadcast_to(perm[b : b + 1, :], (ROWS, LANES))
            for t in range(tiles):
                out[t * ROWS : (t + 1) * ROWS, cols] = jnp.take_along_axis(
                    got[t, b], where, axis=1, mode="promise_in_bounds"
                )
            out[tiles * ROWS : tiles * ROWS + 1, cols] = turned[u : u + 1, :]


def place(got, got_row, perm, width, own_blocks):
    tiles = got.shape[0]
    step = 32
    return pl.pallas_call(
        functools.partial(place_kernel, tiles, step),
        grid=(own_blocks // step,),
        out_shape=jax.ShapeDtypeStruct((width, own_blocks * LANES), jnp.float32),
        in_specs=[
            pl.BlockSpec((tiles, step, ROWS, LANES), lambda i: (0, i, 0, 0)),
            pl.BlockSpec((step, LANES), lambda i: (i, 0)),
            pl.BlockSpec((step, LANES), lambda i: (i, 0)),
        ],
        out_specs=pl.BlockSpec((width, step * LANES), lambda i: (0, i)),
    )(got, got_row, perm)


def advance(state_rows, half_volt, steepness, gate_rate, conductance, reversal):
    voltage = state_rows[0:1]
    gate_vals = state_rows[1:]
    steady = jax.nn.sigmoid((voltage - half_volt[:, None]) * steepness[:, None])
    damping = jnp.exp(-gate_rate[:, None] * (1.0 + jax.nn.sigmoid(voltage)))
    gate_vals = steady + (gate_vals - steady) * damping
    current = jnp.sum(
        conductance[:, None] * gate_vals * (voltage - reversal[:, None]), axis=0, keepdims=True
    )
    voltage = voltage - time_step * current
    return jnp.concatenate([voltage, gate_vals], axis=0)


def general(counts_all, devices, states, block_part, tile_perm, *gate_params):
    d = lax.axis_index(("group", "peer"))
    local_blocks = block_part.shape[0]
    tile_width = tile_perm.shape[1]
    width = states.shape[0]
    capacity = 2 * local_blocks // devices
    partitions = jnp.arange(devices, dtype=jnp.int32)
    onehot = (block_part[:, None] == partitions[None, :]).astype(jnp.int32)
    if counts_all is None:
        counts_all = lax.all_gather(
            jnp.sum(onehot, axis=0, dtype=jnp.int32), ("group", "peer")
        )
    before = (partitions < d).astype(jnp.int32)
    earlier = jnp.sum(counts_all * before[:, None], axis=0, dtype=jnp.int32)
    rank_in = jnp.sum(
        (jnp.cumsum(onehot, axis=0, dtype=jnp.int32) - onehot) * onehot, axis=1, dtype=jnp.int32
    )
    local_index = jnp.sum(onehot * earlier[None, :], axis=1, dtype=jnp.int32) + rank_in
    slot_index = block_part * capacity + rank_in
    requests = jnp.full((devices * capacity,), -1, jnp.int32).at[slot_index].set(local_index)
    requests = requests.reshape(devices, capacity)
    advanced = advance(states, *gate_params)
    advanced = advanced.reshape(width, local_blocks, tile_width)
    wanted = lax.all_to_all(requests, ("group", "peer"), split_axis=0, concat_axis=0, tiled=True)
    picked = jnp.maximum(wanted, 0).reshape(-1)
    served = jnp.take(advanced, picked, axis=1)
    arrived = lax.all_to_all(
        served.reshape(width, wanted.shape[0], wanted.shape[1], tile_width),
        ("group", "peer"), split_axis=1, concat_axis=1, tiled=True,
    )
    flat_cols = (slot_index[:, None] * tile_width + tile_perm).reshape(-1)
    return jnp.take(arrived.reshape(width, devices * capacity * tile_width), flat_cols, axis=1)


def on_device(devices, peers, states, block_part, tile_perm, *gate_params):
    own_blocks = block_part.shape[0]
    width = states.shape[0]
    if (devices, peers) != (4 * ROWS, ROWS) or width % ROWS != 1:
        return general(None, devices, states, block_part, tile_perm, *gate_params)
    tables, tier, counts, own, own_row, ahead = opening(
        block_part.reshape(1, own_blocks), [p.reshape(1, -1) for p in gate_params],
        states, devices, peers,
    )

    def fast(rooms):
        got, got_row = exchange(tables, own, own_row, ahead, peers, own_blocks, rooms)
        return place(got, got_row, tile_perm, width, own_blocks)

    def slow():
        matrix = counts[:, 0, :devices]
        return general(matrix, devices, states, block_part, tile_perm, *gate_params)

    choices = [functools.partial(fast, rooms) for rooms in TIERS] + [slow]
    return lax.switch(tier[0], choices)


def solution(mesh):
    both = P(("group", "peer"))
    return jax.shard_map(
        functools.partial(on_device, mesh.devices.size, mesh.shape["peer"]),
        mesh=mesh,
        in_specs=(P(None, ("group", "peer")), both, P(("group", "peer"), None)) + (P(),) * 5,
        out_specs=P(None, ("group", "peer")),
        check_vma=False,
    )
```

```python
import functools
import jax
import jax.numpy as jnp
import numpy as np
from jax import lax
from jax.experimental import pallas as pl
from jax.experimental.pallas import tpu as pltpu
from jax.sharding import PartitionSpec as P

time_step = 0.25
LANES = 128
ROWS = 8
MESH_ID = pl.DeviceIdType.MESH
VMEM_LIMIT = 67043328
Z_STRIDE = 88
Z_NEAR = 88
P_STRIDE = 48
P_TABLE = 64
PIECES = 4
TIERS = ((72, 40), (80, 40), (88, 48))


def my_index(peers):
    return lax.axis_index("group") * peers + lax.axis_index("peer")


def plane_of(d, peers):
    return (d // peers) * 2 + d % 2


def depth_of(d, peers):
    return (d % peers) // 2


def dot(a, b, contract=((1,), (0,))):
    return lax.dot_general(
        a, b, (contract, ((), ())), preferred_element_type=jnp.float32
    )


def iota(shape, axis):
    return lax.broadcasted_iota(jnp.int32, shape, axis)


def fill_tables(devices, peers, own_blocks, c_ref, part_ref, tab_ref, tier_ref):
    d = my_index(peers)
    plane = plane_of(d, peers)
    depth = depth_of(d, peers)
    planes = ROWS
    depths = peers // 2
    per = own_blocks // planes
    f32 = jnp.float32
    shift = ROWS - 1
    counts = c_ref[...].reshape(devices, LANES)
    lower = (iota((devices, devices), 1) < iota((devices, devices), 0)).astype(f32)
    starts = dot(lower, counts.astype(f32))
    starts_i = starts.astype(jnp.int32)
    upper = (
        iota((own_blocks, own_blocks), 0) < iota((own_blocks, own_blocks), 1)
    ).astype(f32)
    lane = iota((1, own_blocks), 1)
    lane_plane = lane // per
    stored = (lane % per) * planes + (plane ^ lane_plane)
    source_rows = iota((LANES, own_blocks), 0)
    row8 = iota((ROWS, own_blocks), 0)

    def classify(level):
        source = (lane_plane // 2) * peers + level * 2 + lane_plane % 2
        pick = (source_rows == source).astype(f32)
        begin = dot(starts, pick).astype(jnp.int32)
        dest = jnp.sum((begin <= stored).astype(jnp.int32), axis=0, keepdims=True) - 1
        level_to = depth_of(dest, peers)
        mask = (row8 == level_to).astype(f32)
        rank = jnp.sum(mask * dot(mask, upper), axis=0, keepdims=True).astype(jnp.int32)
        return dest, level_to, rank

    tab_ref[...] = jnp.zeros_like(tab_ref)
    _, level_to, rank = classify(depth)
    slots = iota((depths * LANES, own_blocks), 0)
    pick = (slots == level_to * LANES + rank).astype(f32)
    value = jnp.broadcast_to(lane, (ROWS, own_blocks)).astype(f32)
    got = dot(value, pick, ((1,), (1,))).astype(jnp.int32)
    for t in range(depths):
        tab_ref[t : t + 1, :] = got[0:1, t * LANES : (t + 1) * LANES]

    slots = iota((planes * P_TABLE, own_blocks), 0)
    before = jnp.zeros((ROWS, 1), f32)
    table = jnp.zeros((ROWS, planes * P_TABLE), f32)
    for level in range(depths):
        dest, level_to, rank = classify(level)
        here = level_to == depth
        plane_to = plane_of(dest, peers)
        mask = ((row8 == plane_to) & here).astype(f32)
        rank3 = jnp.sum(mask * (dot(mask, upper) + before), axis=0, keepdims=True)
        before = before + jnp.sum(mask, axis=1, keepdims=True)
        key = jnp.where(here, plane_to * P_TABLE + rank3.astype(jnp.int32), -1)
        pick = (slots == key).astype(f32)
        value = jnp.where(row8 == 0, rank, 1).astype(f32)
        got = dot(value, pick, ((1,), (1,)))
        table = table + got + float(level * Z_STRIDE) * got[1:2, :]
    table = table.astype(jnp.int32)
    table = jnp.clip(table, 0, depths * Z_STRIDE - 1)
    wide = planes * P_TABLE // LANES
    for t in range(wide):
        tab_ref[depths + t : depths + t + 1, :] = table[0:1, t * LANES : (t + 1) * LANES]

    part = part_ref[...]
    mine = iota((devices, LANES), 0) == d
    my_start = jnp.sum(jnp.where(mine, starts_i, 0), axis=0, keepdims=True)
    my_count = jnp.sum(jnp.where(mine, counts, 0), axis=0, keepdims=True)
    few = (iota((devices, own_blocks), 0) == part).astype(f32)
    rank = jnp.sum(few * dot(few, upper), axis=0, keepdims=True).astype(jnp.int32)
    pick = (source_rows == part).astype(f32)
    start8 = jnp.broadcast_to(my_start, (ROWS, LANES))
    begin = dot(start8.astype(f32), pick).astype(jnp.int32)[0:1]
    at = begin + rank
    part_plane = plane_of(part, peers)
    middle = (at % planes) ^ part_plane
    ids = iota((1, LANES), 1)
    residue = iota((ROWS, LANES), 0) ^ plane_of(ids, peers)
    in_use = ids < devices
    share = ((start8 + my_count + (shift - residue)) // planes) - (
        (start8 + (shift - residue)) // planes
    )
    share = jnp.where(in_use, share, 0)

    def order_of(p):
        return jnp.where(
            p < devices, depth_of(p, peers) * planes + plane_of(p, peers), LANES
        )

    ahead = (
        order_of(iota((LANES, LANES), 0)) < order_of(iota((LANES, LANES), 1))
    ).astype(f32)
    base = dot(share.astype(f32), ahead)
    base = dot(base, pick)
    base = jnp.sum(jnp.where(row8 == middle, base, 0.0), axis=0, keepdims=True)
    first = (begin + (shift - at % planes)) // planes
    final = middle * P_STRIDE + base.astype(jnp.int32) + at // planes - first
    final = jnp.clip(final, 0, planes * P_STRIDE - 1)
    row = depths + wide
    for t in range(own_blocks // LANES):
        tab_ref[row + t : row + t + 1, :] = final[:, t * LANES : (t + 1) * LANES]

    by_slab = (
        depth_of(iota((ROWS, devices), 1), peers) == iota((ROWS, devices), 0)
    ).astype(f32)
    rows = iota((LANES, LANES), 0)
    by_part = (
        (depth_of(rows, peers) == iota((LANES, LANES), 1)) & (rows < devices)
    ).astype(f32)
    far = ((iota((ROWS, LANES), 0) ^ iota((ROWS, LANES), 1)) & 2) != 0
    level_most = jnp.zeros((ROWS, LANES), f32)
    plane_most = jnp.zeros((devices, 1), f32)
    for k in range(planes):
        left = shift - (k ^ plane_of(ids, peers))
        some = (starts_i + counts + left) // planes - (starts_i + left) // planes
        some = jnp.where(in_use, some, 0).astype(f32)
        plane_most = jnp.maximum(plane_most, jnp.sum(some, axis=1, keepdims=True))
        level_most = jnp.maximum(level_most, dot(dot(by_slab, some), by_part))
    used = jnp.max(jnp.where(far, level_most, 0.0)).astype(jnp.int32)
    most = jnp.max(level_most).astype(jnp.int32)
    final_most = jnp.max(plane_most).astype(jnp.int32)
    tier = jnp.int32(len(TIERS))
    for t in range(len(TIERS) - 1, -1, -1):
        room, room3 = TIERS[t]
        fits = (used <= room) & (final_most <= room3) & (most <= Z_NEAR)
        tier = jnp.where(fits, t, tier)
    tier_ref[0] = tier


def chunk_list(tiles):
    half = ROWS // 2
    chunks = [(0, 0, half), (0, half, half)]
    chunks += [(t, 0, ROWS) for t in range(1, tiles - 1)]
    return chunks + [(tiles - 1, 0, half), (tiles - 1, half, half), (tiles, 0, 1)]


def chunk_shape(chunk, *lead):
    return lead + ((chunk[2], LANES) if chunk[2] > 1 else (LANES,))


def opening_kernel(devices, peers, own_blocks, chunks, *refs):
    (
        part_ref, half_ref, steep_ref, rate_ref, cond_ref, rev_ref, states_ref,
        tab_ref, tier_ref, counts_out, first_out,
    ) = refs[:11]
    refs = refs[11:]
    later = len(chunks) - 1
    own_outs, refs = refs[:later], refs[later:]
    owns, refs = refs[: later + 1], refs[later + 1 :]
    (
        states, params, landed, tally, counts,
        load_sem, count_send, count_recv, send_sem, recv_sem, out_sem,
    ) = refs
    d = my_index(peers)
    plane = plane_of(d, peers)
    depth = depth_of(d, peers)
    planes = ROWS
    tiles = chunks[-1][0]
    per = own_blocks // planes
    step = per // PIECES
    width = step * planes * LANES

    loads = []
    for q in range(PIECES):
        cols = pl.ds(q * width, width)
        copy = pltpu.make_async_copy(
            states_ref.at[:, cols], states.at[:, cols], load_sem.at[q]
        )
        copy.start()
        loads.append(copy)

    barrier = pltpu.get_barrier_semaphore()
    for k in range(1, devices):
        to = (d + k) % devices
        pl.semaphore_signal(
            barrier, inc=1, device_id=(to // peers, to % peers), device_id_type=MESH_ID
        )

    match = (iota((LANES, own_blocks), 0) == part_ref[...]).astype(jnp.float32)
    ones = jnp.ones((ROWS, own_blocks), jnp.float32)
    tally[...] = dot(ones, match, ((1,), (1,)))[0:1].astype(jnp.int32)
    counts[d] = tally[...]
    gates_all = half_ref.shape[1]
    for k, ref in enumerate((half_ref, steep_ref, rate_ref, cond_ref, rev_ref)):
        for base in range(0, tiles * ROWS + ROWS, ROWS):
            shape = (ROWS, gates_all)
            chosen = iota(shape, 1) == iota(shape, 0) + (base - 1)
            column = jnp.sum(jnp.where(chosen, ref[...], 0.0), axis=1, keepdims=True)
            params[k, base : base + ROWS, :] = jnp.broadcast_to(column, (ROWS, LANES))

    def advance_block(i, u):
        cols = pl.ds(pl.multiple_of((i * planes + u) * LANES, LANES), LANES)
        top = states[0:ROWS, cols]
        voltage = top[0:1, :]
        spread = jnp.broadcast_to(voltage, (ROWS, LANES))
        slow = -(1.0 + jax.nn.sigmoid(spread))

        def gates(vals, base, count):
            half, steep, rate, cond, rev = (
                params[k, base : base + count, :] for k in range(5)
            )
            v = spread[0:count]
            steady = jax.nn.sigmoid((v - half) * steep)
            damping = jnp.exp(rate * slow[0:count])
            new = steady + (vals - steady) * damping
            return new, cond * new * (v - rev)

        def keep(tile, value):
            for c, (t, lo, rows) in enumerate(chunks[:-1]):
                if t == tile:
                    if c == 0 and u == 0:
                        landed[plane * per + i] = value[lo : lo + rows]
                    else:
                        owns[c][u, i] = value[lo : lo + rows]

        total = jnp.zeros((ROWS, LANES), jnp.float32)
        for t in range(1, tiles):
            new, term = gates(states[t * ROWS : (t + 1) * ROWS, cols], t * ROWS, ROWS)
            keep(t, new)
            total = total + term
        last = tiles * ROWS
        new_row, term_row = gates(states[last : last + 1, cols], last, 1)
        owns[-1][u, pl.ds(i, 1), :] = new_row
        new, term = gates(top, 0, ROWS)
        total = total + term
        current = jnp.sum(total, axis=0, keepdims=True) + term_row
        moved = voltage - time_step * current
        first = lax.broadcasted_iota(jnp.int32, (ROWS, LANES), 0) == 0
        keep(0, jnp.where(first, jnp.broadcast_to(moved, (ROWS, LANES)), new))

    def advance_loop(i, _):
        for u in range(planes):
            advance_block(i, u)
        return 0

    sends = []
    outs = []
    count_copies = []
    for q in range(PIECES):
        loads[q].wait()
        lax.fori_loop(q * step, (q + 1) * step, advance_loop, 0)
        if q == 0:
            pl.semaphore_wait(barrier, devices - 1)
            for k in range(1, devices):
                to = (d + k) % devices
                copy = pltpu.make_async_remote_copy(
                    src_ref=tally, dst_ref=counts.at[d],
                    send_sem=count_send.at[k], recv_sem=count_recv.at[k],
                    device_id=(to // peers, to % peers), device_id_type=MESH_ID,
                )
                copy.start()
                count_copies.append(copy)
        for m in (6, 7, 4, 5, 1, 3, 2):
            to = plane ^ m
            copy = pltpu.make_async_remote_copy(
                src_ref=owns[0].at[m, pl.ds(q * step, step)],
                dst_ref=landed.at[pl.ds(plane * per + q * step, step)],
                send_sem=send_sem.at[q, m], recv_sem=recv_sem.at[q, m],
                device_id=(to // 2, depth * 2 + to % 2), device_id_type=MESH_ID,
            )
            copy.start()
            sends.append(copy)
        some = pl.ds(q * step, step)
        for c in range(later):
            copy = pltpu.make_async_copy(
                owns[c + 1].at[:, some], own_outs[c].at[:, some], out_sem.at[q, c]
            )
            copy.start()
            outs.append(copy)
    for copy in count_copies:
        copy.wait_recv()
    counts_out[...] = counts[...]
    fill_tables(devices, peers, own_blocks, counts, part_ref, tab_ref, tier_ref)
    for copy in sends:
        copy.wait_recv()
    copy = pltpu.make_async_copy(landed, first_out, out_sem.at[PIECES, 0])
    copy.start()
    outs.append(copy)
    for copy in count_copies + sends:
        copy.wait_send()
    for copy in outs:
        copy.wait()


def opening(part, gate_params, states, devices, peers):
    own_blocks = part.shape[1]
    tiles = states.shape[0] // ROWS
    planes = ROWS
    per = own_blocks // planes
    f32 = jnp.float32
    chunks = chunk_list(tiles)
    vmem = pl.BlockSpec(memory_space=pltpu.VMEM)
    smem = pl.BlockSpec(memory_space=pltpu.SMEM)
    anywhere = pl.BlockSpec(memory_space=pl.ANY)
    owns = [chunk_shape(c, planes, per) for c in chunks]
    first = chunk_shape(chunks[0], own_blocks)
    return pl.pallas_call(
        functools.partial(opening_kernel, devices, peers, own_blocks, chunks),
        out_shape=(
            jax.ShapeDtypeStruct((2 * ROWS, LANES), jnp.int32),
            jax.ShapeDtypeStruct((1,), jnp.int32),
            jax.ShapeDtypeStruct((devices, 1, LANES), jnp.int32),
            jax.ShapeDtypeStruct(first, f32),
            *[jax.ShapeDtypeStruct(o, f32) for o in owns[1:]],
        ),
        in_specs=[vmem] * 6 + [anywhere],
        out_specs=(vmem, smem, vmem, *[anywhere] * len(chunks)),
        scratch_shapes=[
            *[pltpu.VMEM(o, f32) for o in owns],
            pltpu.VMEM(states.shape, f32),
            pltpu.VMEM((5, (tiles + 1) * ROWS, LANES), f32),
            pltpu.VMEM(first, f32),
            pltpu.VMEM((1, LANES), jnp.int32),
            pltpu.VMEM((devices, 1, LANES), jnp.int32),
            pltpu.SemaphoreType.DMA((PIECES,)),
            pltpu.SemaphoreType.DMA((devices,)),
            pltpu.SemaphoreType.DMA((devices,)),
            pltpu.SemaphoreType.DMA((PIECES, planes)),
            pltpu.SemaphoreType.DMA((PIECES, planes)),
            pltpu.SemaphoreType.DMA((PIECES + 1, len(chunks))),
        ],
        compiler_params=pltpu.CompilerParams(
            collective_id=0, has_side_effects=True, vmem_limit_bytes=VMEM_LIMIT
        ),
    )(part, *gate_params, states)


def exchange_kernel(peers, own_blocks, chunks, rooms, tables, perm, ahead, *refs):
    d = my_index(peers)
    plane = plane_of(d, peers)
    depth = depth_of(d, peers)
    planes = ROWS
    depths = peers // 2
    per = own_blocks // planes
    number = len(chunks)
    owns, refs = refs[: number - 1], refs[number - 1 :]
    out, refs = refs[0], refs[1:]
    groups = []
    for _ in range(5):
        groups.append(refs[:number])
        refs = refs[number:]
    landed1, packed2, landed2, packed3, landed3 = groups
    placed, row_ready, send_sem, recv_sem, out_sem, in_sem = refs
    room2, room3 = rooms
    wide = planes * P_TABLE // LANES

    def device(to_plane, to_depth):
        return (to_plane // 2, to_depth * 2 + to_plane % 2)

    barrier = pltpu.get_barrier_semaphore()
    partners = [device(plane ^ m, depth) for m in range(1, planes)]
    partners += [device(plane, depth ^ m) for m in range(1, depths)]
    for to in partners:
        pl.semaphore_signal(barrier, inc=1, device_id=to, device_id_type=MESH_ID)
    loads = [pltpu.make_async_copy(ahead, landed1[0], in_sem.at[0])]
    for c in range(1, number):
        loads.append(
            pltpu.make_async_copy(
                owns[c - 1].at[0], landed1[c].at[pl.ds(plane * per, per)], in_sem.at[c]
            )
        )
    for copy in loads:
        copy.start()
    pl.semaphore_wait(barrier, len(partners))

    def gather(c, count, table_row, table_col, src, put, first):
        unroll = 8

        def body(i, _):
            for u in range(unroll):
                k = i * unroll + u
                where = tables[table_row, table_col + k]
                if chunks[c][2] > 1:
                    put[first + k] = src[where]
                else:
                    put[pl.ds(first + k, 1), :] = src[pl.ds(where, 1), :]
            return 0

        lax.fori_loop(0, count // unroll, body, 0)

    def message(c, phase, m):
        if phase == 0:
            src = owns[c - 1].at[m]
            dst = landed1[c].at[pl.ds(plane * per, per)]
        elif phase == 1:
            room = room2 if not isinstance(m, int) or m > 1 else Z_NEAR
            src = packed2[c].at[m - 1, pl.ds(0, room)]
            dst = landed2[c].at[pl.ds(depth * Z_STRIDE, room)]
        else:
            src = packed3[c].at[m - 1, pl.ds(0, room3)]
            dst = landed3[c].at[pl.ds(plane * P_STRIDE, room3)]
        to = device(plane, depth ^ m) if phase == 1 else device(plane ^ m, depth)
        return pltpu.make_async_remote_copy(
            src_ref=src, dst_ref=dst,
            send_sem=send_sem.at[c, phase, m], recv_sem=recv_sem.at[c, phase, m],
            device_id=to, device_id_type=MESH_ID,
        )

    def phase1(c):
        def body(i, _):
            message(c, 0, planes - 1 - i).start()
            return 0

        lax.fori_loop(0, planes - 1, body, 0)

    def phase2(c):
        loads[c].wait()
        for m in range(1, planes if c else 1):
            message(c, 0, m).wait_recv()

        def body(i, _):
            m = i + 2
            gather(c, room2, depth ^ m, 0, landed1[c], packed2[c].at[m - 1], 0)
            message(c, 1, m).start()
            return 0

        lax.fori_loop(0, depths - 2, body, 0)
        gather(c, Z_NEAR, depth ^ 1, 0, landed1[c], packed2[c].at[0], 0)
        message(c, 1, 1).start()
        gather(c, Z_NEAR, depth, 0, landed1[c], landed2[c], depth * Z_STRIDE)

    def phase3(c):
        for m in range(1, depths):
            message(c, 1, m).wait_recv()

        def body(i, _):
            m = planes - 1 - i
            to = plane ^ m
            gather(
                c, room3, depths + to // 2, (to % 2) * P_TABLE,
                landed2[c], packed3[c].at[m - 1], 0,
            )
            message(c, 2, m).start()
            return 0

        lax.fori_loop(0, planes - 1, body, 0)
        gather(
            c, room3, depths + plane // 2, (plane % 2) * P_TABLE,
            landed2[c], landed3[c], plane * P_STRIDE,
        )

    outs = []

    def turn(values, order):
        return jnp.take_along_axis(values, order, axis=1, mode="promise_in_bounds")

    def finish(c):
        for m in range(1, planes):
            message(c, 2, m).wait_recv()
        tile, low, rows = chunks[c]
        base = tile * ROWS + low
        first = depths + wide

        def body(i, _):
            for u in range(ROWS):
                b = i * ROWS + u
                where = tables[first + b // LANES, b % LANES]
                cols = pl.ds(pl.multiple_of(b * LANES, LANES), LANES)
                order = jnp.broadcast_to(perm[pl.ds(b, 1), :], (rows, LANES))
                placed[base : base + rows, cols] = turn(landed3[c][where], order)
            return 0

        def row_body(i, _):
            eight = pl.ds(pl.multiple_of(i * ROWS, ROWS), ROWS)
            for u in range(ROWS):
                b = i * ROWS + u
                where = tables[first + b // LANES, b % LANES]
                row_ready[u : u + 1, :] = landed3[c][pl.ds(where, 1), :]
            turned = turn(row_ready[...], perm[eight, :])
            for u in range(ROWS):
                cols = pl.ds(pl.multiple_of((i * ROWS + u) * LANES, LANES), LANES)
                placed[base : base + 1, cols] = turned[u : u + 1, :]
            return 0

        lax.fori_loop(0, own_blocks // ROWS, body if rows > 1 else row_body, 0)
        if low + rows == ROWS or rows == 1:
            some = pl.ds(tile * ROWS, low + rows)
            copy = pltpu.make_async_copy(placed.at[some], out.at[some], out_sem.at[tile])
            copy.start()
            outs.append(copy)

    for phase, c in EVENTS:
        (phase1, phase2, phase3, finish)[phase](c)
    for copy in outs:
        copy.wait()
    for c in range(number):
        for m in range(1, planes):
            if c:
                message(c, 0, m).wait_send()
            message(c, 2, m).wait_send()
        for m in range(1, depths):
            message(c, 1, m).wait_send()


EVENTS = (
    (0, 1), (0, 2), (1, 0), (0, 3), (1, 1), (2, 0), (1, 2), (0, 4), (2, 1), (1, 3),
    (0, 5), (0, 6), (0, 7), (3, 0), (1, 4), (2, 2), (3, 1), (1, 5), (1, 6), (1, 7),
    (2, 3), (3, 2), (3, 3), (2, 4), (2, 5), (3, 4), (3, 5), (2, 6), (2, 7), (3, 6), (3, 7),
)


def exchange(tables, perm, ahead, owns, width, peers, own_blocks, rooms):
    planes = ROWS
    depths = peers // 2
    tiles = width // ROWS
    chunks = chunk_list(tiles)
    f32 = jnp.float32

    def buffers(*lead):
        return [pltpu.VMEM(chunk_shape(c, *lead), f32) for c in chunks]

    anywhere = pl.BlockSpec(memory_space=pl.ANY)
    return pl.pallas_call(
        functools.partial(exchange_kernel, peers, own_blocks, chunks, rooms),
        out_shape=jax.ShapeDtypeStruct((width, own_blocks * LANES), f32),
        in_specs=[
            pl.BlockSpec(memory_space=pltpu.SMEM),
            pl.BlockSpec(memory_space=pltpu.VMEM),
            *[anywhere] * len(chunks),
        ],
        out_specs=anywhere,
        scratch_shapes=[
            *buffers(own_blocks),
            *buffers(depths - 1, Z_STRIDE),
            *buffers(depths * Z_STRIDE),
            *buffers(planes - 1, P_STRIDE),
            *buffers(planes * P_STRIDE),
            pltpu.VMEM((width, own_blocks * LANES), f32),
            pltpu.VMEM((ROWS, LANES), f32),
            pltpu.SemaphoreType.DMA((len(chunks), 3, planes)),
            pltpu.SemaphoreType.DMA((len(chunks), 3, planes)),
            pltpu.SemaphoreType.DMA((tiles + 1,)),
            pltpu.SemaphoreType.DMA((len(chunks),)),
        ],
        compiler_params=pltpu.CompilerParams(
            collective_id=1 + TIERS.index(rooms),
            has_side_effects=True,
            vmem_limit_bytes=VMEM_LIMIT,
        ),
    )(tables, perm, ahead, *owns)


def advance(state_rows, half_volt, steepness, gate_rate, conductance, reversal):
    voltage = state_rows[0:1]
    gate_vals = state_rows[1:]
    steady = jax.nn.sigmoid((voltage - half_volt[:, None]) * steepness[:, None])
    damping = jnp.exp(-gate_rate[:, None] * (1.0 + jax.nn.sigmoid(voltage)))
    gate_vals = steady + (gate_vals - steady) * damping
    current = jnp.sum(
        conductance[:, None] * gate_vals * (voltage - reversal[:, None]), axis=0, keepdims=True
    )
    voltage = voltage - time_step * current
    return jnp.concatenate([voltage, gate_vals], axis=0)


def general(counts_all, devices, states, block_part, tile_perm, *gate_params):
    d = lax.axis_index(("group", "peer"))
    local_blocks = block_part.shape[0]
    tile_width = tile_perm.shape[1]
    width = states.shape[0]
    capacity = 2 * local_blocks // devices
    partitions = jnp.arange(devices, dtype=jnp.int32)
    onehot = (block_part[:, None] == partitions[None, :]).astype(jnp.int32)
    if counts_all is None:
        counts_all = lax.all_gather(
            jnp.sum(onehot, axis=0, dtype=jnp.int32), ("group", "peer")
        )
    before = (partitions < d).astype(jnp.int32)
    earlier = jnp.sum(counts_all * before[:, None], axis=0, dtype=jnp.int32)
    rank_in = jnp.sum(
        (jnp.cumsum(onehot, axis=0, dtype=jnp.int32) - onehot) * onehot, axis=1, dtype=jnp.int32
    )
    local_index = jnp.sum(onehot * earlier[None, :], axis=1, dtype=jnp.int32) + rank_in
    slot_index = block_part * capacity + rank_in
    requests = jnp.full((devices * capacity,), -1, jnp.int32).at[slot_index].set(local_index)
    requests = requests.reshape(devices, capacity)
    advanced = advance(states, *gate_params)
    advanced = advanced.reshape(width, local_blocks, tile_width)
    wanted = lax.all_to_all(requests, ("group", "peer"), split_axis=0, concat_axis=0, tiled=True)
    picked = jnp.maximum(wanted, 0).reshape(-1)
    served = jnp.take(advanced, picked, axis=1)
    arrived = lax.all_to_all(
        served.reshape(width, wanted.shape[0], wanted.shape[1], tile_width),
        ("group", "peer"), split_axis=1, concat_axis=1, tiled=True,
    )
    flat_cols = (slot_index[:, None] * tile_width + tile_perm).reshape(-1)
    return jnp.take(arrived.reshape(width, devices * capacity * tile_width), flat_cols, axis=1)


def on_device(devices, peers, states, block_part, tile_perm, *gate_params):
    own_blocks = block_part.shape[0]
    width = states.shape[0]
    if (devices, peers) != (4 * ROWS, ROWS) or width % ROWS != 1:
        return general(None, devices, states, block_part, tile_perm, *gate_params)
    tables, tier, counts, ahead, *owns = opening(
        block_part.reshape(1, own_blocks), [p.reshape(1, -1) for p in gate_params],
        states, devices, peers,
    )

    def fast(rooms):
        return exchange(tables, tile_perm, ahead, owns, width, peers, own_blocks, rooms)

    def slow():
        matrix = counts[:, 0, :devices]
        return general(matrix, devices, states, block_part, tile_perm, *gate_params)

    choices = [functools.partial(fast, rooms) for rooms in TIERS] + [slow]
    return lax.switch(tier[0], choices)


def solution(mesh):
    both = P(("group", "peer"))
    return jax.shard_map(
        functools.partial(on_device, mesh.devices.size, mesh.shape["peer"]),
        mesh=mesh,
        in_specs=(P(None, ("group", "peer")), both, P(("group", "peer"), None)) + (P(),) * 5,
        out_specs=P(None, ("group", "peer")),
        check_vma=False,
    )
```

```python
import functools
import jax
import jax.numpy as jnp
import numpy as np
from jax import lax
from jax.experimental import pallas as pl
from jax.experimental.pallas import tpu as pltpu
from jax.sharding import PartitionSpec as P

time_step = 0.25
LANES = 128
ROWS = 8
MESH_ID = pl.DeviceIdType.MESH
VMEM_LIMIT = 67043328
Z_STRIDE = 88
Z_NEAR = 88
P_STRIDE = 48
P_TABLE = 64
PIECES = 4
TIERS = ((70, 40), (74, 40), (88, 48))


def my_index(peers):
    return lax.axis_index("group") * peers + lax.axis_index("peer")


def plane_of(d, peers):
    return (d // peers) * 2 + d % 2


def depth_of(d, peers):
    return (d % peers) // 2


def dot(a, b, contract=((1,), (0,))):
    return lax.dot_general(
        a, b, (contract, ((), ())), preferred_element_type=jnp.float32
    )


def iota(shape, axis):
    return lax.broadcasted_iota(jnp.int32, shape, axis)


def fill_tables(devices, peers, own_blocks, c_ref, part_ref, tab_ref, tier_ref):
    d = my_index(peers)
    plane = plane_of(d, peers)
    depth = depth_of(d, peers)
    planes = ROWS
    depths = peers // 2
    per = own_blocks // planes
    f32 = jnp.float32
    shift = ROWS - 1
    counts = c_ref[...].reshape(devices, LANES)
    lower = (iota((devices, devices), 1) < iota((devices, devices), 0)).astype(f32)
    starts = dot(lower, counts.astype(f32))
    starts_i = starts.astype(jnp.int32)
    upper = (
        iota((own_blocks, own_blocks), 0) < iota((own_blocks, own_blocks), 1)
    ).astype(f32)
    lane = iota((1, own_blocks), 1)
    lane_plane = lane // per
    stored = (lane % per) * planes + (plane ^ lane_plane)
    source_rows = iota((LANES, own_blocks), 0)
    row8 = iota((ROWS, own_blocks), 0)

    def classify(level):
        source = (lane_plane // 2) * peers + level * 2 + lane_plane % 2
        pick = (source_rows == source).astype(f32)
        begin = dot(starts, pick).astype(jnp.int32)
        dest = jnp.sum((begin <= stored).astype(jnp.int32), axis=0, keepdims=True) - 1
        level_to = depth_of(dest, peers)
        mask = (row8 == level_to).astype(f32)
        rank = jnp.sum(mask * dot(mask, upper), axis=0, keepdims=True).astype(jnp.int32)
        return dest, level_to, rank

    tab_ref[...] = jnp.zeros_like(tab_ref)
    _, level_to, rank = classify(depth)
    slots = iota((depths * LANES, own_blocks), 0)
    pick = (slots == level_to * LANES + rank).astype(f32)
    value = jnp.broadcast_to(lane, (ROWS, own_blocks)).astype(f32)
    got = dot(value, pick, ((1,), (1,))).astype(jnp.int32)
    for t in range(depths):
        tab_ref[t : t + 1, :] = got[0:1, t * LANES : (t + 1) * LANES]

    slots = iota((planes * P_TABLE, own_blocks), 0)
    before = jnp.zeros((ROWS, 1), f32)
    table = jnp.zeros((ROWS, planes * P_TABLE), f32)
    for level in range(depths):
        dest, level_to, rank = classify(level)
        here = level_to == depth
        plane_to = plane_of(dest, peers)
        mask = ((row8 == plane_to) & here).astype(f32)
        rank3 = jnp.sum(mask * (dot(mask, upper) + before), axis=0, keepdims=True)
        before = before + jnp.sum(mask, axis=1, keepdims=True)
        key = jnp.where(here, plane_to * P_TABLE + rank3.astype(jnp.int32), -1)
        pick = (slots == key).astype(f32)
        value = jnp.where(row8 == 0, rank, 1).astype(f32)
        got = dot(value, pick, ((1,), (1,)))
        table = table + got + float(level * Z_STRIDE) * got[1:2, :]
    table = table.astype(jnp.int32)
    table = jnp.clip(table, 0, depths * Z_STRIDE - 1)
    wide = planes * P_TABLE // LANES
    for t in range(wide):
        tab_ref[depths + t : depths + t + 1, :] = table[0:1, t * LANES : (t + 1) * LANES]

    part = part_ref[...]
    mine = iota((devices, LANES), 0) == d
    my_start = jnp.sum(jnp.where(mine, starts_i, 0), axis=0, keepdims=True)
    my_count = jnp.sum(jnp.where(mine, counts, 0), axis=0, keepdims=True)
    few = (iota((devices, own_blocks), 0) == part).astype(f32)
    rank = jnp.sum(few * dot(few, upper), axis=0, keepdims=True).astype(jnp.int32)
    pick = (source_rows == part).astype(f32)
    start8 = jnp.broadcast_to(my_start, (ROWS, LANES))
    begin = dot(start8.astype(f32), pick).astype(jnp.int32)[0:1]
    at = begin + rank
    part_plane = plane_of(part, peers)
    middle = (at % planes) ^ part_plane
    ids = iota((1, LANES), 1)
    residue = iota((ROWS, LANES), 0) ^ plane_of(ids, peers)
    in_use = ids < devices
    share = ((start8 + my_count + (shift - residue)) // planes) - (
        (start8 + (shift - residue)) // planes
    )
    share = jnp.where(in_use, share, 0)

    def order_of(p):
        return jnp.where(
            p < devices, depth_of(p, peers) * planes + plane_of(p, peers), LANES
        )

    ahead = (
        order_of(iota((LANES, LANES), 0)) < order_of(iota((LANES, LANES), 1))
    ).astype(f32)
    base = dot(share.astype(f32), ahead)
    base = dot(base, pick)
    base = jnp.sum(jnp.where(row8 == middle, base, 0.0), axis=0, keepdims=True)
    first = (begin + (shift - at % planes)) // planes
    final = middle * P_STRIDE + base.astype(jnp.int32) + at // planes - first
    final = jnp.clip(final, 0, planes * P_STRIDE - 1)
    row = depths + wide
    for t in range(own_blocks // LANES):
        tab_ref[row + t : row + t + 1, :] = final[:, t * LANES : (t + 1) * LANES]

    by_slab = (
        depth_of(iota((ROWS, devices), 1), peers) == iota((ROWS, devices), 0)
    ).astype(f32)
    rows = iota((LANES, LANES), 0)
    by_part = (
        (depth_of(rows, peers) == iota((LANES, LANES), 1)) & (rows < devices)
    ).astype(f32)
    far = ((iota((ROWS, LANES), 0) ^ iota((ROWS, LANES), 1)) & 2) != 0
    level_most = jnp.zeros((ROWS, LANES), f32)
    plane_most = jnp.zeros((devices, 1), f32)
    for k in range(planes):
        left = shift - (k ^ plane_of(ids, peers))
        some = (starts_i + counts + left) // planes - (starts_i + left) // planes
        some = jnp.where(in_use, some, 0).astype(f32)
        plane_most = jnp.maximum(plane_most, jnp.sum(some, axis=1, keepdims=True))
        level_most = jnp.maximum(level_most, dot(dot(by_slab, some), by_part))
    used = jnp.max(jnp.where(far, level_most, 0.0)).astype(jnp.int32)
    most = jnp.max(level_most).astype(jnp.int32)
    final_most = jnp.max(plane_most).astype(jnp.int32)
    tier = jnp.int32(len(TIERS))
    for t in range(len(TIERS) - 1, -1, -1):
        room, room3 = TIERS[t]
        fits = (used <= room) & (final_most <= room3) & (most <= Z_NEAR)
        tier = jnp.where(fits, t, tier)
    tier_ref[0] = tier


def chunk_list(tiles):
    half = ROWS // 2
    chunks = [(1, 0, half), (1, half, half), (0, 0, ROWS)]
    chunks += [(t, 0, ROWS) for t in range(2, tiles - 1)]
    return chunks + [(tiles - 1, 0, half), (tiles - 1, half, half), (tiles, 0, 1)]


def chunk_shape(chunk, *lead):
    return lead + ((chunk[2], LANES) if chunk[2] > 1 else (LANES,))


def opening_kernel(devices, peers, own_blocks, chunks, *refs):
    (
        part_ref, half_ref, steep_ref, rate_ref, cond_ref, rev_ref, states_ref,
        tab_ref, tier_ref, counts_out, first_out,
    ) = refs[:11]
    refs = refs[11:]
    later = len(chunks) - 1
    own_outs, refs = refs[:later], refs[later:]
    owns, refs = refs[: later + 1], refs[later + 1 :]
    (
        states, params, landed, sums, tally, counts,
        load_sem, count_send, count_recv, send_sem, recv_sem, out_sem,
    ) = refs
    d = my_index(peers)
    plane = plane_of(d, peers)
    depth = depth_of(d, peers)
    planes = ROWS
    tiles = chunks[-1][0]
    per = own_blocks // planes
    step = per // PIECES
    width = step * planes * LANES

    lead = 2 * ROWS
    height = states_ref.shape[0]
    loads = []
    for part, (low, high) in enumerate(((0, lead), (lead, height))):
        for q in range(PIECES):
            some = (pl.ds(low, high - low), pl.ds(q * width, width))
            copy = pltpu.make_async_copy(
                states_ref.at[some], states.at[some], load_sem.at[part, q]
            )
            copy.start()
            loads.append(copy)

    barrier = pltpu.get_barrier_semaphore()
    for k in range(1, devices):
        to = (d + k) % devices
        pl.semaphore_signal(
            barrier, inc=1, device_id=(to // peers, to % peers), device_id_type=MESH_ID
        )

    match = (iota((LANES, own_blocks), 0) == part_ref[...]).astype(jnp.float32)
    ones = jnp.ones((ROWS, own_blocks), jnp.float32)
    tally[...] = dot(ones, match, ((1,), (1,)))[0:1].astype(jnp.int32)
    counts[d] = tally[...]
    gates_all = half_ref.shape[1]
    for k, ref in enumerate((half_ref, steep_ref, rate_ref, cond_ref, rev_ref)):
        for base in range(0, tiles * ROWS + ROWS, ROWS):
            shape = (ROWS, gates_all)
            chosen = iota(shape, 1) == iota(shape, 0) + (base - 1)
            column = jnp.sum(jnp.where(chosen, ref[...], 0.0), axis=1, keepdims=True)
            params[k, base : base + ROWS, :] = jnp.broadcast_to(column, (ROWS, LANES))

    def columns(i, u):
        return pl.ds(pl.multiple_of((i * planes + u) * LANES, LANES), LANES)

    def spread_of(cols):
        spread = jnp.broadcast_to(states[0:1, cols], (ROWS, LANES))
        return spread, -(1.0 + jax.nn.sigmoid(spread))

    def gates(spread, slow, cols, base, count):
        half, steep, rate, cond, rev = (
            params[k, base : base + count, :] for k in range(5)
        )
        vals = states[base : base + count, cols]
        v = spread[0:count]
        steady = jax.nn.sigmoid((v - half) * steep)
        damping = jnp.exp(rate * slow[0:count])
        new = steady + (vals - steady) * damping
        return new, cond * new * (v - rev)

    def keep(tile, value, i, u):
        for c, (t, lo, rows) in enumerate(chunks[:-1]):
            if t == tile:
                if c == 0 and u == 0:
                    landed[plane * per + i] = value[lo : lo + rows]
                else:
                    owns[c][u, i] = value[lo : lo + rows]

    def early_loop(i, _):
        for u in range(planes):
            cols = columns(i, u)
            spread, slow = spread_of(cols)
            new, term = gates(spread, slow, cols, ROWS, ROWS)
            keep(1, new, i, u)
            sums[i * planes + u] = term
        return 0

    def advance_block(i, u):
        cols = columns(i, u)
        spread, slow = spread_of(cols)
        total = sums[i * planes + u]
        for t in range(2, tiles):
            new, term = gates(spread, slow, cols, t * ROWS, ROWS)
            keep(t, new, i, u)
            total = total + term
        last = tiles * ROWS
        new_row, term_row = gates(spread, slow, cols, last, 1)
        owns[-1][u, pl.ds(i, 1), :] = new_row
        new, term = gates(spread, slow, cols, 0, ROWS)
        total = total + term
        current = jnp.sum(total, axis=0, keepdims=True) + term_row
        moved = states[0:1, cols] - time_step * current
        first = lax.broadcasted_iota(jnp.int32, (ROWS, LANES), 0) == 0
        keep(0, jnp.where(first, jnp.broadcast_to(moved, (ROWS, LANES)), new), i, u)

    def advance_loop(i, _):
        for u in range(planes):
            advance_block(i, u)
        return 0

    sends = []
    outs = []
    count_copies = []
    for q in range(PIECES):
        loads[q].wait()
        lax.fori_loop(q * step, (q + 1) * step, early_loop, 0)
        if q == 0:
            pl.semaphore_wait(barrier, devices - 1)
            for k in range(1, devices):
                to = (d + k) % devices
                copy = pltpu.make_async_remote_copy(
                    src_ref=tally, dst_ref=counts.at[d],
                    send_sem=count_send.at[k], recv_sem=count_recv.at[k],
                    device_id=(to // peers, to % peers), device_id_type=MESH_ID,
                )
                copy.start()
                count_copies.append(copy)
        for m in (6, 7, 4, 5, 1, 3, 2):
            to = plane ^ m
            copy = pltpu.make_async_remote_copy(
                src_ref=owns[0].at[m, pl.ds(q * step, step)],
                dst_ref=landed.at[pl.ds(plane * per + q * step, step)],
                send_sem=send_sem.at[q, m], recv_sem=recv_sem.at[q, m],
                device_id=(to // 2, depth * 2 + to % 2), device_id_type=MESH_ID,
            )
            copy.start()
            sends.append(copy)
    for q in range(PIECES):
        loads[PIECES + q].wait()
        lax.fori_loop(q * step, (q + 1) * step, advance_loop, 0)
        some = pl.ds(q * step, step)
        for c in range(later):
            copy = pltpu.make_async_copy(
                owns[c + 1].at[:, some], own_outs[c].at[:, some], out_sem.at[q, c]
            )
            copy.start()
            outs.append(copy)
    for copy in count_copies:
        copy.wait_recv()
    counts_out[...] = counts[...]
    fill_tables(devices, peers, own_blocks, counts, part_ref, tab_ref, tier_ref)
    for copy in sends:
        copy.wait_recv()
    copy = pltpu.make_async_copy(landed, first_out, out_sem.at[PIECES, 0])
    copy.start()
    outs.append(copy)
    for copy in count_copies + sends:
        copy.wait_send()
    for copy in outs:
        copy.wait()


def opening(part, gate_params, states, devices, peers):
    own_blocks = part.shape[1]
    tiles = states.shape[0] // ROWS
    planes = ROWS
    per = own_blocks // planes
    f32 = jnp.float32
    chunks = chunk_list(tiles)
    vmem = pl.BlockSpec(memory_space=pltpu.VMEM)
    smem = pl.BlockSpec(memory_space=pltpu.SMEM)
    anywhere = pl.BlockSpec(memory_space=pl.ANY)
    owns = [chunk_shape(c, planes, per) for c in chunks]
    first = chunk_shape(chunks[0], own_blocks)
    return pl.pallas_call(
        functools.partial(opening_kernel, devices, peers, own_blocks, chunks),
        out_shape=(
            jax.ShapeDtypeStruct((2 * ROWS, LANES), jnp.int32),
            jax.ShapeDtypeStruct((1,), jnp.int32),
            jax.ShapeDtypeStruct((devices, 1, LANES), jnp.int32),
            jax.ShapeDtypeStruct(first, f32),
            *[jax.ShapeDtypeStruct(o, f32) for o in owns[1:]],
        ),
        in_specs=[vmem] * 6 + [anywhere],
        out_specs=(vmem, smem, vmem, *[anywhere] * len(chunks)),
        scratch_shapes=[
            *[pltpu.VMEM(o, f32) for o in owns],
            pltpu.VMEM(states.shape, f32),
            pltpu.VMEM((5, (tiles + 1) * ROWS, LANES), f32),
            pltpu.VMEM(first, f32),
            pltpu.VMEM((own_blocks, ROWS, LANES), f32),
            pltpu.VMEM((1, LANES), jnp.int32),
            pltpu.VMEM((devices, 1, LANES), jnp.int32),
            pltpu.SemaphoreType.DMA((2, PIECES)),
            pltpu.SemaphoreType.DMA((devices,)),
            pltpu.SemaphoreType.DMA((devices,)),
            pltpu.SemaphoreType.DMA((PIECES, planes)),
            pltpu.SemaphoreType.DMA((PIECES, planes)),
            pltpu.SemaphoreType.DMA((PIECES + 1, len(chunks))),
        ],
        compiler_params=pltpu.CompilerParams(
            collective_id=0, has_side_effects=True, vmem_limit_bytes=VMEM_LIMIT
        ),
    )(part, *gate_params, states)


def exchange_kernel(peers, own_blocks, chunks, rooms, tables, ahead, *refs):
    d = my_index(peers)
    plane = plane_of(d, peers)
    depth = depth_of(d, peers)
    planes = ROWS
    depths = peers // 2
    per = own_blocks // planes
    number = len(chunks)
    owns, refs = refs[: number - 1], refs[number - 1 :]
    out, out_row, refs = refs[0], refs[1], refs[2:]
    groups = []
    for _ in range(5):
        groups.append(refs[:number])
        refs = refs[number:]
    landed1, packed2, landed2, packed3, landed3 = groups
    ready, ready_row, send_sem, recv_sem, out_sem, in_sem = refs
    near, room3 = Z_NEAR, rooms[1]
    wide = planes * P_TABLE // LANES

    def device(to_plane, to_depth):
        return (to_plane // 2, to_depth * 2 + to_plane % 2)

    barrier = pltpu.get_barrier_semaphore()
    partners = [device(plane ^ m, depth) for m in range(1, planes)]
    partners += [device(plane, depth ^ m) for m in range(1, depths)]
    for to in partners:
        pl.semaphore_signal(barrier, inc=1, device_id=to, device_id_type=MESH_ID)
    loads = [pltpu.make_async_copy(ahead, landed1[0], in_sem.at[0])]
    for c in range(1, number):
        loads.append(
            pltpu.make_async_copy(
                owns[c - 1].at[0], landed1[c].at[pl.ds(plane * per, per)], in_sem.at[c]
            )
        )
    for copy in loads:
        copy.start()
    pl.semaphore_wait(barrier, len(partners))

    def gather(c, count, table_row, table_col, src, put, first):
        unroll = 8

        def body(i, _):
            for u in range(unroll):
                k = i * unroll + u
                where = tables[table_row, table_col + k]
                if chunks[c][2] > 1:
                    put[first + k] = src[where]
                else:
                    put[pl.ds(first + k, 1), :] = src[pl.ds(where, 1), :]
            return 0

        lax.fori_loop(0, count // unroll, body, 0)

    def message(c, phase, m):
        if phase == 0:
            src = owns[c - 1].at[m]
            dst = landed1[c].at[pl.ds(plane * per, per)]
        elif phase == 1:
            room = near if m == 1 else rooms[0]
            room = room if chunks[c][2] > 1 else -(-room // ROWS) * ROWS
            src = packed2[c].at[m - 1, pl.ds(0, room)]
            dst = landed2[c].at[pl.ds(depth * Z_STRIDE, room)]
        else:
            src = packed3[c].at[m - 1, pl.ds(0, room3)]
            dst = landed3[c].at[pl.ds(plane * P_STRIDE, room3)]
        to = device(plane, depth ^ m) if phase == 1 else device(plane ^ m, depth)
        return pltpu.make_async_remote_copy(
            src_ref=src, dst_ref=dst,
            send_sem=send_sem.at[c, phase, m], recv_sem=recv_sem.at[c, phase, m],
            device_id=to, device_id_type=MESH_ID,
        )

    def phase1(c):
        def body(i, _):
            message(c, 0, planes - 1 - i).start()
            return 0

        lax.fori_loop(0, planes - 1, body, 0)

    waited = set()

    def arrive(c, phase, m):
        if (c, phase, m) not in waited:
            waited.add((c, phase, m))
            message(c, phase, m).wait_recv()

    def phase2(c, gate):
        loads[c].wait()
        for m in range(1, planes if c else 1):
            arrive(c, 0, m)
        for m in (2, 3, 1):
            if gate is not None:
                arrive(gate, 1, m)
            room = near if m == 1 else -(-rooms[0] // ROWS) * ROWS
            gather(c, room, depth ^ m, 0, landed1[c], packed2[c].at[m - 1], 0)
            message(c, 1, m).start()
        gather(c, near, depth, 0, landed1[c], landed2[c], depth * Z_STRIDE)

    def phase3(c):
        for m in range(1, depths):
            arrive(c, 1, m)

        def body(i, _):
            m = planes - 1 - i
            to = plane ^ m
            gather(
                c, room3, depths + to // 2, (to % 2) * P_TABLE,
                landed2[c], packed3[c].at[m - 1], 0,
            )
            message(c, 2, m).start()
            return 0

        lax.fori_loop(0, planes - 1, body, 0)
        gather(
            c, room3, depths + plane // 2, (plane % 2) * P_TABLE,
            landed2[c], landed3[c], plane * P_STRIDE,
        )

    outs = []

    def finish(c):
        for m in range(1, planes):
            arrive(c, 2, m)
        tile, low, rows = chunks[c]
        first = depths + wide

        def body(i, _):
            for u in range(ROWS):
                b = i * ROWS + u
                where = tables[first + b // LANES, b % LANES]
                if rows > 1:
                    ready[tile, b, low : low + rows] = landed3[c][where]
                else:
                    ready_row[pl.ds(b, 1), :] = landed3[c][pl.ds(where, 1), :]
            return 0

        lax.fori_loop(0, own_blocks // ROWS, body, 0)
        if rows == 1:
            copy = pltpu.make_async_copy(ready_row, out_row, out_sem.at[tile])
        elif low + rows == ROWS:
            copy = pltpu.make_async_copy(ready.at[tile], out.at[tile], out_sem.at[tile])
        else:
            return
        copy.start()
        outs.append(copy)

    for phase, *c in EVENTS:
        (phase1, phase2, phase3, finish)[phase](*c)
    for copy in outs:
        copy.wait()
    for c in range(number):
        for m in range(1, planes):
            if c:
                message(c, 0, m).wait_send()
            message(c, 2, m).wait_send()
        for m in range(1, depths):
            message(c, 1, m).wait_send()


EVENTS = (
    (0, 1), (1, 0, None), (0, 2), (0, 3), (1, 1, 0), (2, 0), (1, 2, 1), (0, 4), (2, 1),
    (1, 3, 2), (3, 0), (0, 5), (0, 6), (0, 7), (2, 2), (1, 4, 3), (3, 1), (2, 3), (3, 2),
    (1, 5, 4), (2, 4), (1, 6, 5), (1, 7, None), (3, 3), (2, 5), (3, 4), (2, 6), (2, 7),
    (3, 5), (3, 6), (3, 7),
)


def exchange(tables, ahead, owns, width, peers, own_blocks, rooms):
    planes = ROWS
    depths = peers // 2
    tiles = width // ROWS
    chunks = chunk_list(tiles)
    f32 = jnp.float32

    def buffers(*lead):
        return [pltpu.VMEM(chunk_shape(c, *lead), f32) for c in chunks]

    anywhere = pl.BlockSpec(memory_space=pl.ANY)
    return pl.pallas_call(
        functools.partial(exchange_kernel, peers, own_blocks, chunks, rooms),
        out_shape=(
            jax.ShapeDtypeStruct((tiles, own_blocks, ROWS, LANES), f32),
            jax.ShapeDtypeStruct((own_blocks, LANES), f32),
        ),
        in_specs=[pl.BlockSpec(memory_space=pltpu.SMEM), *[anywhere] * len(chunks)],
        out_specs=(anywhere, anywhere),
        scratch_shapes=[
            *buffers(own_blocks),
            *buffers(depths - 1, Z_STRIDE),
            *buffers(depths * Z_STRIDE),
            *buffers(planes - 1, P_STRIDE),
            *buffers(planes * P_STRIDE),
            pltpu.VMEM((tiles, own_blocks, ROWS, LANES), f32),
            pltpu.VMEM((own_blocks, LANES), f32),
            pltpu.SemaphoreType.DMA((len(chunks), 3, planes)),
            pltpu.SemaphoreType.DMA((len(chunks), 3, planes)),
            pltpu.SemaphoreType.DMA((tiles + 1,)),
            pltpu.SemaphoreType.DMA((len(chunks),)),
        ],
        compiler_params=pltpu.CompilerParams(
            collective_id=1 + TIERS.index(rooms),
            has_side_effects=True,
            vmem_limit_bytes=VMEM_LIMIT,
        ),
    )(tables, ahead, *owns)


def place_kernel(tiles, blocks, got, got_row, perm, out):
    def body(group, _):
        rows = pl.ds(pl.multiple_of(group * ROWS, ROWS), ROWS)
        orders = perm[rows, :]
        turned = jnp.take_along_axis(
            got_row[rows, :], orders, axis=1, mode="promise_in_bounds"
        )
        for u in range(ROWS):
            b = group * ROWS + u
            cols = pl.ds(pl.multiple_of(b * LANES, LANES), LANES)
            where = jnp.broadcast_to(orders[u : u + 1, :], (ROWS, LANES))
            for t in range(tiles):
                out[t * ROWS : (t + 1) * ROWS, cols] = jnp.take_along_axis(
                    got[t, b], where, axis=1, mode="promise_in_bounds"
                )
            out[tiles * ROWS : tiles * ROWS + 1, cols] = turned[u : u + 1, :]
        return 0

    lax.fori_loop(0, blocks // ROWS, body, 0, unroll=2)


def place(got, got_row, perm, width, own_blocks):
    tiles = got.shape[0]
    step = 64
    return pl.pallas_call(
        functools.partial(place_kernel, tiles, step),
        grid=(own_blocks // step,),
        out_shape=jax.ShapeDtypeStruct((width, own_blocks * LANES), jnp.float32),
        in_specs=[
            pl.BlockSpec((tiles, step, ROWS, LANES), lambda i: (0, i, 0, 0)),
            pl.BlockSpec((step, LANES), lambda i: (i, 0)),
            pl.BlockSpec((step, LANES), lambda i: (i, 0)),
        ],
        out_specs=pl.BlockSpec((width, step * LANES), lambda i: (0, i)),
    )(got, got_row, perm)


def advance(state_rows, half_volt, steepness, gate_rate, conductance, reversal):
    voltage = state_rows[0:1]
    gate_vals = state_rows[1:]
    steady = jax.nn.sigmoid((voltage - half_volt[:, None]) * steepness[:, None])
    damping = jnp.exp(-gate_rate[:, None] * (1.0 + jax.nn.sigmoid(voltage)))
    gate_vals = steady + (gate_vals - steady) * damping
    current = jnp.sum(
        conductance[:, None] * gate_vals * (voltage - reversal[:, None]), axis=0, keepdims=True
    )
    voltage = voltage - time_step * current
    return jnp.concatenate([voltage, gate_vals], axis=0)


def general(counts_all, devices, states, block_part, tile_perm, *gate_params):
    d = lax.axis_index(("group", "peer"))
    local_blocks = block_part.shape[0]
    tile_width = tile_perm.shape[1]
    width = states.shape[0]
    capacity = 2 * local_blocks // devices
    partitions = jnp.arange(devices, dtype=jnp.int32)
    onehot = (block_part[:, None] == partitions[None, :]).astype(jnp.int32)
    if counts_all is None:
        counts_all = lax.all_gather(
            jnp.sum(onehot, axis=0, dtype=jnp.int32), ("group", "peer")
        )
    before = (partitions < d).astype(jnp.int32)
    earlier = jnp.sum(counts_all * before[:, None], axis=0, dtype=jnp.int32)
    rank_in = jnp.sum(
        (jnp.cumsum(onehot, axis=0, dtype=jnp.int32) - onehot) * onehot, axis=1, dtype=jnp.int32
    )
    local_index = jnp.sum(onehot * earlier[None, :], axis=1, dtype=jnp.int32) + rank_in
    slot_index = block_part * capacity + rank_in
    requests = jnp.full((devices * capacity,), -1, jnp.int32).at[slot_index].set(local_index)
    requests = requests.reshape(devices, capacity)
    advanced = advance(states, *gate_params)
    advanced = advanced.reshape(width, local_blocks, tile_width)
    wanted = lax.all_to_all(requests, ("group", "peer"), split_axis=0, concat_axis=0, tiled=True)
    picked = jnp.maximum(wanted, 0).reshape(-1)
    served = jnp.take(advanced, picked, axis=1)
    arrived = lax.all_to_all(
        served.reshape(width, wanted.shape[0], wanted.shape[1], tile_width),
        ("group", "peer"), split_axis=1, concat_axis=1, tiled=True,
    )
    flat_cols = (slot_index[:, None] * tile_width + tile_perm).reshape(-1)
    return jnp.take(arrived.reshape(width, devices * capacity * tile_width), flat_cols, axis=1)


def on_device(devices, peers, states, block_part, tile_perm, *gate_params):
    own_blocks = block_part.shape[0]
    width = states.shape[0]
    if (devices, peers) != (4 * ROWS, ROWS) or width % ROWS != 1:
        return general(None, devices, states, block_part, tile_perm, *gate_params)
    tables, tier, counts, ahead, *owns = opening(
        block_part.reshape(1, own_blocks), [p.reshape(1, -1) for p in gate_params],
        states, devices, peers,
    )

    def fast(rooms):
        got, got_row = exchange(tables, ahead, owns, width, peers, own_blocks, rooms)
        return place(got, got_row, tile_perm, width, own_blocks)

    def slow():
        matrix = counts[:, 0, :devices]
        return general(matrix, devices, states, block_part, tile_perm, *gate_params)

    choices = [functools.partial(fast, rooms) for rooms in TIERS] + [slow]
    return lax.switch(tier[0], choices)


def solution(mesh):
    both = P(("group", "peer"))
    return jax.shard_map(
        functools.partial(on_device, mesh.devices.size, mesh.shape["peer"]),
        mesh=mesh,
        in_specs=(P(None, ("group", "peer")), both, P(("group", "peer"), None)) + (P(),) * 5,
        out_specs=P(None, ("group", "peer")),
        check_vma=False,
    )
```

```python
import functools
import jax
import jax.numpy as jnp
import numpy as np
from jax import lax
from jax.experimental import pallas as pl
from jax.experimental.pallas import tpu as pltpu
from jax.sharding import PartitionSpec as P

time_step = 0.25
LANES = 128
ROWS = 8
MESH_ID = pl.DeviceIdType.MESH
VMEM_LIMIT = 67043328
Z_STRIDE = 88
P_STRIDE = 48
P_TABLE = 64
PIECES = 4
TIERS = ((70, 74, 40), (74, 78, 40), (84, 88, 48))


def my_index(peers):
    return lax.axis_index("group") * peers + lax.axis_index("peer")


def plane_of(d, peers):
    return (d // peers) * 2 + d % 2


def depth_of(d, peers):
    return (d % peers) // 2


def dot(a, b, contract=((1,), (0,))):
    return lax.dot_general(
        a, b, (contract, ((), ())), preferred_element_type=jnp.float32
    )


def iota(shape, axis):
    return lax.broadcasted_iota(jnp.int32, shape, axis)


def fill_tables(devices, peers, own_blocks, c_ref, part_ref, tab_ref, tier_ref):
    d = my_index(peers)
    plane = plane_of(d, peers)
    depth = depth_of(d, peers)
    planes = ROWS
    depths = peers // 2
    per = own_blocks // planes
    f32 = jnp.float32
    shift = ROWS - 1
    counts = c_ref[...].reshape(devices, LANES)
    lower = (iota((devices, devices), 1) < iota((devices, devices), 0)).astype(f32)
    starts = dot(lower, counts.astype(f32))
    starts_i = starts.astype(jnp.int32)
    upper = (
        iota((own_blocks, own_blocks), 0) < iota((own_blocks, own_blocks), 1)
    ).astype(f32)
    lane = iota((1, own_blocks), 1)
    lane_plane = lane // per
    stored = (lane % per) * planes + (plane ^ lane_plane)
    source_rows = iota((LANES, own_blocks), 0)
    row8 = iota((ROWS, own_blocks), 0)

    def classify(level):
        source = (lane_plane // 2) * peers + level * 2 + lane_plane % 2
        pick = (source_rows == source).astype(f32)
        begin = dot(starts, pick).astype(jnp.int32)
        dest = jnp.sum((begin <= stored).astype(jnp.int32), axis=0, keepdims=True) - 1
        level_to = depth_of(dest, peers)
        mask = (row8 == level_to).astype(f32)
        rank = jnp.sum(mask * dot(mask, upper), axis=0, keepdims=True).astype(jnp.int32)
        return dest, level_to, rank

    tab_ref[...] = jnp.zeros_like(tab_ref)
    _, level_to, rank = classify(depth)
    slots = iota((depths * LANES, own_blocks), 0)
    pick = (slots == level_to * LANES + rank).astype(f32)
    value = jnp.broadcast_to(lane, (ROWS, own_blocks)).astype(f32)
    got = dot(value, pick, ((1,), (1,))).astype(jnp.int32)
    for t in range(depths):
        tab_ref[t : t + 1, :] = got[0:1, t * LANES : (t + 1) * LANES]

    slots = iota((planes * P_TABLE, own_blocks), 0)
    before = jnp.zeros((ROWS, 1), f32)
    table = jnp.zeros((ROWS, planes * P_TABLE), f32)
    for level in range(depths):
        dest, level_to, rank = classify(level)
        here = level_to == depth
        plane_to = plane_of(dest, peers)
        mask = ((row8 == plane_to) & here).astype(f32)
        rank3 = jnp.sum(mask * (dot(mask, upper) + before), axis=0, keepdims=True)
        before = before + jnp.sum(mask, axis=1, keepdims=True)
        key = jnp.where(here, plane_to * P_TABLE + rank3.astype(jnp.int32), -1)
        pick = (slots == key).astype(f32)
        value = jnp.where(row8 == 0, rank, 1).astype(f32)
        got = dot(value, pick, ((1,), (1,)))
        table = table + got + float(level * Z_STRIDE) * got[1:2, :]
    table = table.astype(jnp.int32)
    table = jnp.clip(table, 0, depths * Z_STRIDE - 1)
    wide = planes * P_TABLE // LANES
    for t in range(wide):
        tab_ref[depths + t : depths + t + 1, :] = table[0:1, t * LANES : (t + 1) * LANES]

    part = part_ref[...]
    mine = iota((devices, LANES), 0) == d
    my_start = jnp.sum(jnp.where(mine, starts_i, 0), axis=0, keepdims=True)
    my_count = jnp.sum(jnp.where(mine, counts, 0), axis=0, keepdims=True)
    few = (iota((devices, own_blocks), 0) == part).astype(f32)
    rank = jnp.sum(few * dot(few, upper), axis=0, keepdims=True).astype(jnp.int32)
    pick = (source_rows == part).astype(f32)
    start8 = jnp.broadcast_to(my_start, (ROWS, LANES))
    begin = dot(start8.astype(f32), pick).astype(jnp.int32)[0:1]
    at = begin + rank
    part_plane = plane_of(part, peers)
    middle = (at % planes) ^ part_plane
    ids = iota((1, LANES), 1)
    residue = iota((ROWS, LANES), 0) ^ plane_of(ids, peers)
    in_use = ids < devices
    share = ((start8 + my_count + (shift - residue)) // planes) - (
        (start8 + (shift - residue)) // planes
    )
    share = jnp.where(in_use, share, 0)

    def order_of(p):
        return jnp.where(
            p < devices, depth_of(p, peers) * planes + plane_of(p, peers), LANES
        )

    ahead = (
        order_of(iota((LANES, LANES), 0)) < order_of(iota((LANES, LANES), 1))
    ).astype(f32)
    base = dot(share.astype(f32), ahead)
    base = dot(base, pick)
    base = jnp.sum(jnp.where(row8 == middle, base, 0.0), axis=0, keepdims=True)
    first = (begin + (shift - at % planes)) // planes
    final = middle * P_STRIDE + base.astype(jnp.int32) + at // planes - first
    final = jnp.clip(final, 0, planes * P_STRIDE - 1)
    row = depths + wide
    for t in range(own_blocks // LANES):
        tab_ref[row + t : row + t + 1, :] = final[:, t * LANES : (t + 1) * LANES]

    by_slab = (
        depth_of(iota((ROWS, devices), 1), peers) == iota((ROWS, devices), 0)
    ).astype(f32)
    rows = iota((LANES, LANES), 0)
    by_part = (
        (depth_of(rows, peers) == iota((LANES, LANES), 1)) & (rows < devices)
    ).astype(f32)
    far = ((iota((ROWS, LANES), 0) ^ iota((ROWS, LANES), 1)) & 2) != 0
    level_most = jnp.zeros((ROWS, LANES), f32)
    plane_most = jnp.zeros((devices, 1), f32)
    for k in range(planes):
        left = shift - (k ^ plane_of(ids, peers))
        some = (starts_i + counts + left) // planes - (starts_i + left) // planes
        some = jnp.where(in_use, some, 0).astype(f32)
        plane_most = jnp.maximum(plane_most, jnp.sum(some, axis=1, keepdims=True))
        level_most = jnp.maximum(level_most, dot(dot(by_slab, some), by_part))
    used = jnp.max(jnp.where(far, level_most, 0.0)).astype(jnp.int32)
    most = jnp.max(level_most).astype(jnp.int32)
    final_most = jnp.max(plane_most).astype(jnp.int32)
    tier = jnp.int32(len(TIERS))
    for t in range(len(TIERS) - 1, -1, -1):
        room, near, room3 = TIERS[t]
        fits = (used <= room) & (final_most <= room3) & (most <= near)
        tier = jnp.where(fits, t, tier)
    tier_ref[0] = tier


def chunk_list(tiles):
    half = ROWS // 2
    chunks = [(1, 0, half), (1, half, half), (0, 0, ROWS)]
    chunks += [(t, 0, ROWS) for t in range(2, tiles - 1)]
    return chunks + [(tiles - 1, 0, half), (tiles - 1, half, half), (tiles, 0, 1)]


def chunk_shape(chunk, *lead):
    return lead + ((chunk[2], LANES) if chunk[2] > 1 else (LANES,))


def block_columns(i, u):
    return pl.ds(pl.multiple_of((i * ROWS + u) * LANES, LANES), LANES)


def spread_of(states, cols):
    spread = jnp.broadcast_to(states[0:1, cols], (ROWS, LANES))
    return spread, -(1.0 + jax.nn.sigmoid(spread))


def gates(states, params, spread, slow, cols, base, count):
    half, steep, rate, cond, rev = (
        params[k, base : base + count, :] for k in range(5)
    )
    vals = states[base : base + count, cols]
    v = spread[0:count]
    steady = jax.nn.sigmoid((v - half) * steep)
    damping = jnp.exp(rate * slow[0:count])
    new = steady + (vals - steady) * damping
    return new, cond * new * (v - rev)


def opening_kernel(devices, peers, own_blocks, chunks, *refs):
    (
        part_ref, half_ref, steep_ref, rate_ref, cond_ref, rev_ref, states_ref,
        tab_ref, tier_ref, counts_out, params, first_out, next_out,
        own, own_next, states, landed, tally, counts,
        load_sem, count_send, count_recv, send_sem, recv_sem, out_sem,
    ) = refs
    d = my_index(peers)
    plane = plane_of(d, peers)
    depth = depth_of(d, peers)
    planes = ROWS
    tiles = chunks[-1][0]
    per = own_blocks // planes
    step = per // PIECES
    width = step * planes * LANES

    loads = []
    for q in range(PIECES):
        some = (pl.ds(0, 2 * ROWS), pl.ds(q * width, width))
        copy = pltpu.make_async_copy(
            states_ref.at[some], states.at[some], load_sem.at[q]
        )
        copy.start()
        loads.append(copy)

    barrier = pltpu.get_barrier_semaphore()
    for k in range(1, devices):
        to = (d + k) % devices
        pl.semaphore_signal(
            barrier, inc=1, device_id=(to // peers, to % peers), device_id_type=MESH_ID
        )

    match = (iota((LANES, own_blocks), 0) == part_ref[...]).astype(jnp.float32)
    ones = jnp.ones((ROWS, own_blocks), jnp.float32)
    tally[...] = dot(ones, match, ((1,), (1,)))[0:1].astype(jnp.int32)
    counts[d] = tally[...]
    gates_all = half_ref.shape[1]
    for k, ref in enumerate((half_ref, steep_ref, rate_ref, cond_ref, rev_ref)):
        for base in range(0, tiles * ROWS + ROWS, ROWS):
            shape = (ROWS, gates_all)
            chosen = iota(shape, 1) == iota(shape, 0) + (base - 1)
            column = jnp.sum(jnp.where(chosen, ref[...], 0.0), axis=1, keepdims=True)
            params[k, base : base + ROWS, :] = jnp.broadcast_to(column, (ROWS, LANES))

    half = chunks[0][2]

    def early_loop(i, _):
        for u in range(planes):
            cols = block_columns(i, u)
            spread, slow = spread_of(states, cols)
            new, _ = gates(states, params, spread, slow, cols, ROWS, ROWS)
            if u == 0:
                landed[plane * per + i] = new[0:half]
            else:
                own[u, i] = new[0:half]
            own_next[u, i] = new[half:ROWS]
        return 0

    sends = []
    outs = []
    count_copies = []
    for q in range(PIECES):
        loads[q].wait()
        lax.fori_loop(q * step, (q + 1) * step, early_loop, 0)
        if q == 0:
            pl.semaphore_wait(barrier, devices - 1)
            for k in range(1, devices):
                to = (d + k) % devices
                copy = pltpu.make_async_remote_copy(
                    src_ref=tally, dst_ref=counts.at[d],
                    send_sem=count_send.at[k], recv_sem=count_recv.at[k],
                    device_id=(to // peers, to % peers), device_id_type=MESH_ID,
                )
                copy.start()
                count_copies.append(copy)
        for m in (6, 7, 4, 5, 1, 3, 2):
            to = plane ^ m
            copy = pltpu.make_async_remote_copy(
                src_ref=own.at[m, pl.ds(q * step, step)],
                dst_ref=landed.at[pl.ds(plane * per + q * step, step)],
                send_sem=send_sem.at[q, m], recv_sem=recv_sem.at[q, m],
                device_id=(to // 2, depth * 2 + to % 2), device_id_type=MESH_ID,
            )
            copy.start()
            sends.append(copy)
    copy = pltpu.make_async_copy(own_next, next_out, out_sem.at[0])
    copy.start()
    outs.append(copy)
    for copy in count_copies:
        copy.wait_recv()
    counts_out[...] = counts[...]
    fill_tables(devices, peers, own_blocks, counts, part_ref, tab_ref, tier_ref)
    for copy in sends:
        copy.wait_recv()
    copy = pltpu.make_async_copy(landed, first_out, out_sem.at[1])
    copy.start()
    outs.append(copy)
    for copy in count_copies + sends:
        copy.wait_send()
    for copy in outs:
        copy.wait()


def opening(part, gate_params, states, devices, peers):
    own_blocks = part.shape[1]
    tiles = states.shape[0] // ROWS
    planes = ROWS
    per = own_blocks // planes
    f32 = jnp.float32
    chunks = chunk_list(tiles)
    vmem = pl.BlockSpec(memory_space=pltpu.VMEM)
    smem = pl.BlockSpec(memory_space=pltpu.SMEM)
    anywhere = pl.BlockSpec(memory_space=pl.ANY)
    first = chunk_shape(chunks[0], own_blocks)
    own = chunk_shape(chunks[0], planes, per)
    own_next = chunk_shape(chunks[1], planes, per)
    params = (5, (tiles + 1) * ROWS, LANES)
    return pl.pallas_call(
        functools.partial(opening_kernel, devices, peers, own_blocks, chunks),
        out_shape=(
            jax.ShapeDtypeStruct((2 * ROWS, LANES), jnp.int32),
            jax.ShapeDtypeStruct((1,), jnp.int32),
            jax.ShapeDtypeStruct((devices, 1, LANES), jnp.int32),
            jax.ShapeDtypeStruct(params, f32),
            jax.ShapeDtypeStruct(first, f32),
            jax.ShapeDtypeStruct(own_next, f32),
        ),
        in_specs=[vmem] * 6 + [anywhere],
        out_specs=(vmem, smem, vmem, vmem, anywhere, anywhere),
        scratch_shapes=[
            pltpu.VMEM(own, f32),
            pltpu.VMEM(own_next, f32),
            pltpu.VMEM((2 * ROWS, states.shape[1]), f32),
            pltpu.VMEM(first, f32),
            pltpu.VMEM((1, LANES), jnp.int32),
            pltpu.VMEM((devices, 1, LANES), jnp.int32),
            pltpu.SemaphoreType.DMA((PIECES,)),
            pltpu.SemaphoreType.DMA((devices,)),
            pltpu.SemaphoreType.DMA((devices,)),
            pltpu.SemaphoreType.DMA((PIECES, planes)),
            pltpu.SemaphoreType.DMA((PIECES, planes)),
            pltpu.SemaphoreType.DMA((2,)),
        ],
        compiler_params=pltpu.CompilerParams(
            collective_id=0, has_side_effects=True, vmem_limit_bytes=VMEM_LIMIT
        ),
    )(part, *gate_params, states)


def exchange_kernel(peers, own_blocks, chunks, rooms, tables, params, states_ref, ahead, behind, *refs):
    d = my_index(peers)
    plane = plane_of(d, peers)
    depth = depth_of(d, peers)
    planes = ROWS
    depths = peers // 2
    per = own_blocks // planes
    number = len(chunks)
    tiles = chunks[-1][0]
    out, out_row, states, refs = refs[0], refs[1], refs[2], refs[3:]
    owns, refs = (None, behind, *refs[: number - 2]), refs[number - 2 :]
    groups = []
    for _ in range(5):
        groups.append(refs[:number])
        refs = refs[number:]
    landed1, packed2, landed2, packed3, landed3 = groups
    ready, ready_row, send_sem, recv_sem, out_sem, in_sem = refs
    room2, near, room3 = rooms
    wide = planes * P_TABLE // LANES

    def device(to_plane, to_depth):
        return (to_plane // 2, to_depth * 2 + to_plane % 2)

    barrier = pltpu.get_barrier_semaphore()
    partners = [device(plane ^ m, depth) for m in range(1, planes)]
    partners += [device(plane, depth ^ m) for m in range(1, depths)]
    for to in partners:
        pl.semaphore_signal(barrier, inc=1, device_id=to, device_id_type=MESH_ID)
    loads = [
        pltpu.make_async_copy(ahead, landed1[0], in_sem.at[0]),
        pltpu.make_async_copy(
            behind.at[0], landed1[1].at[pl.ds(plane * per, per)], in_sem.at[1]
        ),
        pltpu.make_async_copy(states_ref, states, in_sem.at[2]),
    ]
    for copy in loads:
        copy.start()
    pl.semaphore_wait(barrier, len(partners))

    def gather(c, count, table_row, table_col, src, put, first):
        unroll = 8

        def body(i, _):
            for u in range(unroll):
                k = i * unroll + u
                where = tables[table_row, table_col + k]
                if chunks[c][2] > 1:
                    put[first + k] = src[where]
                else:
                    put[pl.ds(first + k, 1), :] = src[pl.ds(where, 1), :]
            return 0

        lax.fori_loop(0, count // unroll, body, 0)

    def whole(room):
        return -(-room // ROWS) * ROWS

    def message(c, phase, m):
        if phase == 0:
            src = owns[c].at[m]
            dst = landed1[c].at[pl.ds(plane * per, per)]
        elif phase == 1:
            room = near if isinstance(m, int) and m == 1 else room2
            room = room if chunks[c][2] > 1 else whole(room)
            src = packed2[c].at[m - 1, pl.ds(0, room)]
            dst = landed2[c].at[pl.ds(depth * Z_STRIDE, room)]
        else:
            src = packed3[c].at[m - 1, pl.ds(0, room3)]
            dst = landed3[c].at[pl.ds(plane * P_STRIDE, room3)]
        to = device(plane, depth ^ m) if phase == 1 else device(plane ^ m, depth)
        return pltpu.make_async_remote_copy(
            src_ref=src, dst_ref=dst,
            send_sem=send_sem.at[c, phase, m], recv_sem=recv_sem.at[c, phase, m],
            device_id=to, device_id_type=MESH_ID,
        )

    def phase1(c):
        def body(i, _):
            message(c, 0, planes - 1 - i).start()
            return 0

        lax.fori_loop(0, planes - 1, body, 0)

    def keep(tile, value, i, u):
        for c, (t, low, rows) in enumerate(chunks):
            if t == tile and c > 1:
                if rows == 1 and u == 0:
                    landed1[c][pl.ds(plane * per + i, 1), :] = value
                elif rows == 1:
                    owns[c][u, pl.ds(i, 1), :] = value
                elif u == 0:
                    landed1[c][plane * per + i] = value[low : low + rows]
                else:
                    owns[c][u, i] = value[low : low + rows]

    def advance_block(i, u):
        cols = block_columns(i, u)
        spread, slow = spread_of(states, cols)
        total = jnp.zeros((ROWS, LANES), jnp.float32)
        for t in range(1, tiles):
            new, term = gates(states, params, spread, slow, cols, t * ROWS, ROWS)
            keep(t, new, i, u)
            total = total + term
        new_row, term_row = gates(states, params, spread, slow, cols, tiles * ROWS, 1)
        keep(tiles, new_row, i, u)
        new, term = gates(states, params, spread, slow, cols, 0, ROWS)
        total = total + term
        current = jnp.sum(total, axis=0, keepdims=True) + term_row
        moved = states[0:1, cols] - time_step * current
        first = lax.broadcasted_iota(jnp.int32, (ROWS, LANES), 0) == 0
        keep(0, jnp.where(first, jnp.broadcast_to(moved, (ROWS, LANES)), new), i, u)

    def advance_rest():
        loads[2].wait()

        def body(i, _):
            for u in range(planes):
                advance_block(i, u)
            return 0

        lax.fori_loop(0, per, body, 0)

    waited = set()

    def arrive(c, phase, m):
        if (c, phase, m) not in waited:
            waited.add((c, phase, m))
            message(c, phase, m).wait_recv()

    def phase2(c, gate):
        if c < 2:
            loads[c].wait()
        for m in range(1, planes if c else 1):
            arrive(c, 0, m)

        def body(i, _):
            m = depths - 1 - i
            if gate is not None:
                message(gate, 1, m).wait_recv()
            gather(c, whole(room2), depth ^ m, 0, landed1[c], packed2[c].at[m - 1], 0)
            message(c, 1, m).start()
            return 0

        lax.fori_loop(0, depths - 2, body, 0)
        if gate is not None:
            waited.update((gate, 1, m) for m in range(2, depths))
            arrive(gate, 1, 1)
        gather(c, whole(near), depth ^ 1, 0, landed1[c], packed2[c].at[0], 0)
        message(c, 1, 1).start()
        gather(c, whole(near), depth, 0, landed1[c], landed2[c], depth * Z_STRIDE)

    def phase3(c):
        for m in range(1, depths):
            arrive(c, 1, m)

        def body(i, _):
            m = planes - 1 - i
            to = plane ^ m
            gather(
                c, room3, depths + to // 2, (to % 2) * P_TABLE,
                landed2[c], packed3[c].at[m - 1], 0,
            )
            message(c, 2, m).start()
            return 0

        lax.fori_loop(0, planes - 1, body, 0)
        gather(
            c, room3, depths + plane // 2, (plane % 2) * P_TABLE,
            landed2[c], landed3[c], plane * P_STRIDE,
        )

    outs = []

    def finish(c):
        for m in range(1, planes):
            arrive(c, 2, m)
        tile, low, rows = chunks[c]
        first = depths + wide

        def body(i, _):
            for u in range(ROWS):
                b = i * ROWS + u
                where = tables[first + b // LANES, b % LANES]
                if rows > 1:
                    ready[tile, b, low : low + rows] = landed3[c][where]
                else:
                    ready_row[pl.ds(b, 1), :] = landed3[c][pl.ds(where, 1), :]
            return 0

        lax.fori_loop(0, own_blocks // ROWS, body, 0)
        if rows == 1:
            copy = pltpu.make_async_copy(ready_row, out_row, out_sem.at[tile])
        elif low + rows == ROWS:
            copy = pltpu.make_async_copy(ready.at[tile], out.at[tile], out_sem.at[tile])
        else:
            return
        copy.start()
        outs.append(copy)

    for phase, *c in EVENTS:
        (phase1, phase2, phase3, finish, advance_rest)[phase](*c)
    for copy in outs:
        copy.wait()
    for c in range(number):
        for m in range(1, planes):
            if c:
                message(c, 0, m).wait_send()
            message(c, 2, m).wait_send()
        for m in range(1, depths):
            message(c, 1, m).wait_send()


EVENTS = (
    (0, 1), (1, 0, None), (4,), (0, 2), (0, 3), (1, 1, 0), (2, 0), (1, 2, 1), (0, 4), (2, 1),
    (1, 3, 2), (3, 0), (0, 5), (0, 6), (0, 7), (2, 2), (1, 4, 3), (3, 1), (2, 3), (3, 2),
    (1, 5, 4), (2, 4), (1, 6, 5), (1, 7, None), (3, 3), (2, 5), (3, 4), (2, 6), (2, 7),
    (3, 5), (3, 6), (3, 7),
)


def exchange(tables, params, states, ahead, behind, peers, own_blocks, rooms):
    width = states.shape[0]
    per = own_blocks // ROWS
    planes = ROWS
    depths = peers // 2
    tiles = width // ROWS
    chunks = chunk_list(tiles)
    f32 = jnp.float32

    def buffers(*lead):
        return [pltpu.VMEM(chunk_shape(c, *lead), f32) for c in chunks]

    anywhere = pl.BlockSpec(memory_space=pl.ANY)
    return pl.pallas_call(
        functools.partial(exchange_kernel, peers, own_blocks, chunks, rooms),
        out_shape=(
            jax.ShapeDtypeStruct((tiles, own_blocks, ROWS, LANES), f32),
            jax.ShapeDtypeStruct((own_blocks, LANES), f32),
        ),
        in_specs=[
            pl.BlockSpec(memory_space=pltpu.SMEM),
            pl.BlockSpec(memory_space=pltpu.VMEM),
            anywhere, anywhere, anywhere,
        ],
        out_specs=(anywhere, anywhere),
        scratch_shapes=[
            pltpu.VMEM(states.shape, f32),
            *buffers(planes, per)[2:],
            *buffers(own_blocks),
            *buffers(depths - 1, Z_STRIDE),
            *buffers(depths * Z_STRIDE),
            *buffers(planes - 1, P_STRIDE),
            *buffers(planes * P_STRIDE),
            pltpu.VMEM((tiles, own_blocks, ROWS, LANES), f32),
            pltpu.VMEM((own_blocks, LANES), f32),
            pltpu.SemaphoreType.DMA((len(chunks), 3, planes)),
            pltpu.SemaphoreType.DMA((len(chunks), 3, planes)),
            pltpu.SemaphoreType.DMA((tiles + 1,)),
            pltpu.SemaphoreType.DMA((3,)),
        ],
        compiler_params=pltpu.CompilerParams(
            collective_id=1 + TIERS.index(rooms),
            has_side_effects=True,
            vmem_limit_bytes=VMEM_LIMIT,
        ),
    )(tables, params, states, ahead, behind)


def place_kernel(tiles, blocks, got, got_row, perm, out):
    def body(group, _):
        rows = pl.ds(pl.multiple_of(group * ROWS, ROWS), ROWS)
        orders = perm[rows, :]
        turned = jnp.take_along_axis(
            got_row[rows, :], orders, axis=1, mode="promise_in_bounds"
        )
        for u in range(ROWS):
            b = group * ROWS + u
            cols = pl.ds(pl.multiple_of(b * LANES, LANES), LANES)
            where = jnp.broadcast_to(orders[u : u + 1, :], (ROWS, LANES))
            for t in range(tiles):
                out[t * ROWS : (t + 1) * ROWS, cols] = jnp.take_along_axis(
                    got[t, b], where, axis=1, mode="promise_in_bounds"
                )
            out[tiles * ROWS : tiles * ROWS + 1, cols] = turned[u : u + 1, :]
        return 0

    lax.fori_loop(0, blocks // ROWS, body, 0, unroll=2)


def place(got, got_row, perm, width, own_blocks):
    tiles = got.shape[0]
    step = 64
    return pl.pallas_call(
        functools.partial(place_kernel, tiles, step),
        grid=(own_blocks // step,),
        out_shape=jax.ShapeDtypeStruct((width, own_blocks * LANES), jnp.float32),
        in_specs=[
            pl.BlockSpec((tiles, step, ROWS, LANES), lambda i: (0, i, 0, 0)),
            pl.BlockSpec((step, LANES), lambda i: (i, 0)),
            pl.BlockSpec((step, LANES), lambda i: (i, 0)),
        ],
        out_specs=pl.BlockSpec((width, step * LANES), lambda i: (0, i)),
    )(got, got_row, perm)


def advance(state_rows, half_volt, steepness, gate_rate, conductance, reversal):
    voltage = state_rows[0:1]
    gate_vals = state_rows[1:]
    steady = jax.nn.sigmoid((voltage - half_volt[:, None]) * steepness[:, None])
    damping = jnp.exp(-gate_rate[:, None] * (1.0 + jax.nn.sigmoid(voltage)))
    gate_vals = steady + (gate_vals - steady) * damping
    current = jnp.sum(
        conductance[:, None] * gate_vals * (voltage - reversal[:, None]), axis=0, keepdims=True
    )
    voltage = voltage - time_step * current
    return jnp.concatenate([voltage, gate_vals], axis=0)


def general(counts_all, devices, states, block_part, tile_perm, *gate_params):
    d = lax.axis_index(("group", "peer"))
    local_blocks = block_part.shape[0]
    tile_width = tile_perm.shape[1]
    width = states.shape[0]
    capacity = 2 * local_blocks // devices
    partitions = jnp.arange(devices, dtype=jnp.int32)
    onehot = (block_part[:, None] == partitions[None, :]).astype(jnp.int32)
    if counts_all is None:
        counts_all = lax.all_gather(
            jnp.sum(onehot, axis=0, dtype=jnp.int32), ("group", "peer")
        )
    before = (partitions < d).astype(jnp.int32)
    earlier = jnp.sum(counts_all * before[:, None], axis=0, dtype=jnp.int32)
    rank_in = jnp.sum(
        (jnp.cumsum(onehot, axis=0, dtype=jnp.int32) - onehot) * onehot, axis=1, dtype=jnp.int32
    )
    local_index = jnp.sum(onehot * earlier[None, :], axis=1, dtype=jnp.int32) + rank_in
    slot_index = block_part * capacity + rank_in
    requests = jnp.full((devices * capacity,), -1, jnp.int32).at[slot_index].set(local_index)
    requests = requests.reshape(devices, capacity)
    advanced = advance(states, *gate_params)
    advanced = advanced.reshape(width, local_blocks, tile_width)
    wanted = lax.all_to_all(requests, ("group", "peer"), split_axis=0, concat_axis=0, tiled=True)
    picked = jnp.maximum(wanted, 0).reshape(-1)
    served = jnp.take(advanced, picked, axis=1)
    arrived = lax.all_to_all(
        served.reshape(width, wanted.shape[0], wanted.shape[1], tile_width),
        ("group", "peer"), split_axis=1, concat_axis=1, tiled=True,
    )
    flat_cols = (slot_index[:, None] * tile_width + tile_perm).reshape(-1)
    return jnp.take(arrived.reshape(width, devices * capacity * tile_width), flat_cols, axis=1)


def on_device(devices, peers, states, block_part, tile_perm, *gate_params):
    own_blocks = block_part.shape[0]
    width = states.shape[0]
    if (devices, peers) != (4 * ROWS, ROWS) or width % ROWS != 1:
        return general(None, devices, states, block_part, tile_perm, *gate_params)
    tables, tier, counts, params, ahead, behind = opening(
        block_part.reshape(1, own_blocks), [p.reshape(1, -1) for p in gate_params],
        states, devices, peers,
    )

    def fast(rooms):
        got, got_row = exchange(
            tables, params, states, ahead, behind, peers, own_blocks, rooms
        )
        return place(got, got_row, tile_perm, width, own_blocks)

    def slow():
        matrix = counts[:, 0, :devices]
        return general(matrix, devices, states, block_part, tile_perm, *gate_params)

    choices = [functools.partial(fast, rooms) for rooms in TIERS] + [slow]
    return lax.switch(tier[0], choices)


def solution(mesh):
    both = P(("group", "peer"))
    return jax.shard_map(
        functools.partial(on_device, mesh.devices.size, mesh.shape["peer"]),
        mesh=mesh,
        in_specs=(P(None, ("group", "peer")), both, P(("group", "peer"), None)) + (P(),) * 5,
        out_specs=P(None, ("group", "peer")),
        check_vma=False,
    )
```

```python
import functools
import jax
import jax.numpy as jnp
import numpy as np
from jax import lax
from jax.experimental import pallas as pl
from jax.experimental.pallas import tpu as pltpu
from jax.sharding import PartitionSpec as P

time_step = 0.25
LANES = 128
ROWS = 8
MESH_ID = pl.DeviceIdType.MESH
VMEM_LIMIT = 67043328
Z_STRIDE = 88
P_STRIDE = 48
P_TABLE = 64
PIECES = 4
TIERS = ((70, 74, 40), (72, 76, 40), (76, 80, 40), (84, 88, 48))


def my_index(peers):
    return lax.axis_index("group") * peers + lax.axis_index("peer")


def plane_of(d, peers):
    return (d // peers) * 2 + d % 2


def depth_of(d, peers):
    return (d % peers) // 2


def dot(a, b, contract=((1,), (0,))):
    return lax.dot_general(
        a, b, (contract, ((), ())), preferred_element_type=jnp.float32
    )


def iota(shape, axis):
    return lax.broadcasted_iota(jnp.int32, shape, axis)


def fill_tables(devices, peers, own_blocks, c_ref, part_ref, tab_ref, tier_ref):
    d = my_index(peers)
    plane = plane_of(d, peers)
    depth = depth_of(d, peers)
    planes = ROWS
    depths = peers // 2
    per = own_blocks // planes
    f32 = jnp.float32
    shift = ROWS - 1
    counts = c_ref[...].reshape(devices, LANES)
    lower = (iota((devices, devices), 1) < iota((devices, devices), 0)).astype(f32)
    starts = dot(lower, counts.astype(f32))
    starts_i = starts.astype(jnp.int32)
    upper = (
        iota((own_blocks, own_blocks), 0) < iota((own_blocks, own_blocks), 1)
    ).astype(f32)
    lane = iota((1, own_blocks), 1)
    lane_plane = lane // per
    stored = (lane % per) * planes + (plane ^ lane_plane)
    source_rows = iota((LANES, own_blocks), 0)
    row8 = iota((ROWS, own_blocks), 0)

    def classify(level):
        source = (lane_plane // 2) * peers + level * 2 + lane_plane % 2
        pick = (source_rows == source).astype(f32)
        begin = dot(starts, pick).astype(jnp.int32)
        dest = jnp.sum((begin <= stored).astype(jnp.int32), axis=0, keepdims=True) - 1
        level_to = depth_of(dest, peers)
        mask = (row8 == level_to).astype(f32)
        rank = jnp.sum(mask * dot(mask, upper), axis=0, keepdims=True).astype(jnp.int32)
        return dest, level_to, rank

    tab_ref[...] = jnp.zeros_like(tab_ref)
    _, level_to, rank = classify(depth)
    slots = iota((depths * LANES, own_blocks), 0)
    pick = (slots == level_to * LANES + rank).astype(f32)
    value = jnp.broadcast_to(lane, (ROWS, own_blocks)).astype(f32)
    got = dot(value, pick, ((1,), (1,))).astype(jnp.int32)
    for t in range(depths):
        tab_ref[t : t + 1, :] = got[0:1, t * LANES : (t + 1) * LANES]

    slots = iota((planes * P_TABLE, own_blocks), 0)
    before = jnp.zeros((ROWS, 1), f32)
    table = jnp.zeros((ROWS, planes * P_TABLE), f32)
    for level in range(depths):
        dest, level_to, rank = classify(level)
        here = level_to == depth
        plane_to = plane_of(dest, peers)
        mask = ((row8 == plane_to) & here).astype(f32)
        rank3 = jnp.sum(mask * (dot(mask, upper) + before), axis=0, keepdims=True)
        before = before + jnp.sum(mask, axis=1, keepdims=True)
        key = jnp.where(here, plane_to * P_TABLE + rank3.astype(jnp.int32), -1)
        pick = (slots == key).astype(f32)
        value = jnp.where(row8 == 0, rank, 1).astype(f32)
        got = dot(value, pick, ((1,), (1,)))
        table = table + got + float(level * Z_STRIDE) * got[1:2, :]
    table = table.astype(jnp.int32)
    table = jnp.clip(table, 0, depths * Z_STRIDE - 1)
    wide = planes * P_TABLE // LANES
    for t in range(wide):
        tab_ref[depths + t : depths + t + 1, :] = table[0:1, t * LANES : (t + 1) * LANES]

    part = part_ref[...]
    mine = iota((devices, LANES), 0) == d
    my_start = jnp.sum(jnp.where(mine, starts_i, 0), axis=0, keepdims=True)
    my_count = jnp.sum(jnp.where(mine, counts, 0), axis=0, keepdims=True)
    few = (iota((devices, own_blocks), 0) == part).astype(f32)
    rank = jnp.sum(few * dot(few, upper), axis=0, keepdims=True).astype(jnp.int32)
    pick = (source_rows == part).astype(f32)
    start8 = jnp.broadcast_to(my_start, (ROWS, LANES))
    begin = dot(start8.astype(f32), pick).astype(jnp.int32)[0:1]
    at = begin + rank
    part_plane = plane_of(part, peers)
    middle = (at % planes) ^ part_plane
    ids = iota((1, LANES), 1)
    residue = iota((ROWS, LANES), 0) ^ plane_of(ids, peers)
    in_use = ids < devices
    share = ((start8 + my_count + (shift - residue)) // planes) - (
        (start8 + (shift - residue)) // planes
    )
    share = jnp.where(in_use, share, 0)

    def order_of(p):
        return jnp.where(
            p < devices, depth_of(p, peers) * planes + plane_of(p, peers), LANES
        )

    ahead = (
        order_of(iota((LANES, LANES), 0)) < order_of(iota((LANES, LANES), 1))
    ).astype(f32)
    base = dot(share.astype(f32), ahead)
    base = dot(base, pick)
    base = jnp.sum(jnp.where(row8 == middle, base, 0.0), axis=0, keepdims=True)
    first = (begin + (shift - at % planes)) // planes
    final = middle * P_STRIDE + base.astype(jnp.int32) + at // planes - first
    final = jnp.clip(final, 0, planes * P_STRIDE - 1)
    row = depths + wide
    for t in range(own_blocks // LANES):
        tab_ref[row + t : row + t + 1, :] = final[:, t * LANES : (t + 1) * LANES]

    by_slab = (
        depth_of(iota((ROWS, devices), 1), peers) == iota((ROWS, devices), 0)
    ).astype(f32)
    rows = iota((LANES, LANES), 0)
    by_part = (
        (depth_of(rows, peers) == iota((LANES, LANES), 1)) & (rows < devices)
    ).astype(f32)
    far = ((iota((ROWS, LANES), 0) ^ iota((ROWS, LANES), 1)) & 2) != 0
    level_most = jnp.zeros((ROWS, LANES), f32)
    plane_most = jnp.zeros((devices, 1), f32)
    for k in range(planes):
        left = shift - (k ^ plane_of(ids, peers))
        some = (starts_i + counts + left) // planes - (starts_i + left) // planes
        some = jnp.where(in_use, some, 0).astype(f32)
        plane_most = jnp.maximum(plane_most, jnp.sum(some, axis=1, keepdims=True))
        level_most = jnp.maximum(level_most, dot(dot(by_slab, some), by_part))
    used = jnp.max(jnp.where(far, level_most, 0.0)).astype(jnp.int32)
    most = jnp.max(level_most).astype(jnp.int32)
    final_most = jnp.max(plane_most).astype(jnp.int32)
    tier = jnp.int32(len(TIERS))
    for t in range(len(TIERS) - 1, -1, -1):
        room, near, room3 = TIERS[t]
        fits = (used <= room) & (final_most <= room3) & (most <= near)
        tier = jnp.where(fits, t, tier)
    tier_ref[0] = tier


def chunk_list(tiles):
    half = ROWS // 2
    chunks = [(1, 0, half), (1, half, half), (0, 0, ROWS)]
    chunks += [(t, 0, ROWS) for t in range(2, tiles - 1)]
    return chunks + [(tiles - 1, 0, half), (tiles - 1, half, half), (tiles, 0, 1)]


def chunk_shape(chunk, *lead):
    return lead + ((chunk[2], LANES) if chunk[2] > 1 else (LANES,))


def repeat(low, high, step):
    def body(i, _):
        step(i)
        return 0

    lax.fori_loop(low, high, body, 0)


def block_columns(i, u):
    return pl.ds(pl.multiple_of((i * ROWS + u) * LANES, LANES), LANES)


def spread_of(states, cols):
    spread = jnp.broadcast_to(states[0:1, cols], (ROWS, LANES))
    return spread, -(1.0 + jax.nn.sigmoid(spread))


def gates(states, params, spread, slow, cols, base, count):
    half, steep, rate, cond, rev = (
        params[k, base : base + count, :] for k in range(5)
    )
    vals = states[base : base + count, cols]
    v = spread[0:count]
    steady = jax.nn.sigmoid((v - half) * steep)
    damping = jnp.exp(rate * slow[0:count])
    new = steady + (vals - steady) * damping
    return new, cond * new * (v - rev)


def opening_kernel(devices, peers, own_blocks, chunks, *refs):
    (
        part_ref, half_ref, steep_ref, rate_ref, cond_ref, rev_ref, states_ref,
        tab_ref, tier_ref, counts_out, params, first_out, next_out,
        own, own_next, states, landed, tally, counts,
        load_sem, count_send, count_recv, send_sem, recv_sem, out_sem,
    ) = refs
    d = my_index(peers)
    plane = plane_of(d, peers)
    depth = depth_of(d, peers)
    planes = ROWS
    tiles = chunks[-1][0]
    per = own_blocks // planes
    step = per // PIECES
    width = step * planes * LANES

    loads = []
    for q in range(PIECES):
        some = (pl.ds(0, 2 * ROWS), pl.ds(q * width, width))
        copy = pltpu.make_async_copy(
            states_ref.at[some], states.at[some], load_sem.at[q]
        )
        copy.start()
        loads.append(copy)

    barrier = pltpu.get_barrier_semaphore()

    def greet(k):
        to = (d + k) % devices
        pl.semaphore_signal(
            barrier, inc=1, device_id=(to // peers, to % peers), device_id_type=MESH_ID
        )

    def count_message(k):
        to = (d + k) % devices
        return pltpu.make_async_remote_copy(
            src_ref=tally, dst_ref=counts.at[d],
            send_sem=count_send.at[k], recv_sem=count_recv.at[k],
            device_id=(to // peers, to % peers), device_id_type=MESH_ID,
        )

    repeat(1, devices, greet)

    match = (iota((LANES, own_blocks), 0) == part_ref[...]).astype(jnp.float32)
    ones = jnp.ones((ROWS, own_blocks), jnp.float32)
    tally[...] = dot(ones, match, ((1,), (1,)))[0:1].astype(jnp.int32)
    counts[d] = tally[...]
    gates_all = half_ref.shape[1]
    for k, ref in enumerate((half_ref, steep_ref, rate_ref, cond_ref, rev_ref)):
        for base in range(0, tiles * ROWS + ROWS, ROWS):
            shape = (ROWS, gates_all)
            chosen = iota(shape, 1) == iota(shape, 0) + (base - 1)
            column = jnp.sum(jnp.where(chosen, ref[...], 0.0), axis=1, keepdims=True)
            params[k, base : base + ROWS, :] = jnp.broadcast_to(column, (ROWS, LANES))

    half = chunks[0][2]

    def early_loop(i, _):
        for u in range(planes):
            cols = block_columns(i, u)
            spread, slow = spread_of(states, cols)
            new, _ = gates(states, params, spread, slow, cols, ROWS, ROWS)
            if u == 0:
                landed[plane * per + i] = new[0:half]
            else:
                own[u, i] = new[0:half]
            own_next[u, i] = new[half:ROWS]
        return 0

    sends = []
    outs = []
    for q in range(PIECES):
        loads[q].wait()
        lax.fori_loop(q * step, (q + 1) * step, early_loop, 0)
        if q == 0:
            pl.semaphore_wait(barrier, devices - 1)
            repeat(1, devices, lambda k: count_message(k).start())
        for m in (6, 7, 4, 5, 1, 3, 2):
            to = plane ^ m
            copy = pltpu.make_async_remote_copy(
                src_ref=own.at[m, pl.ds(q * step, step)],
                dst_ref=landed.at[pl.ds(plane * per + q * step, step)],
                send_sem=send_sem.at[q, m], recv_sem=recv_sem.at[q, m],
                device_id=(to // 2, depth * 2 + to % 2), device_id_type=MESH_ID,
            )
            copy.start()
            sends.append(copy)
    copy = pltpu.make_async_copy(own_next, next_out, out_sem.at[0])
    copy.start()
    outs.append(copy)
    repeat(1, devices, lambda k: count_message(k).wait_recv())
    counts_out[...] = counts[...]
    fill_tables(devices, peers, own_blocks, counts, part_ref, tab_ref, tier_ref)
    for copy in sends:
        copy.wait_recv()
    copy = pltpu.make_async_copy(landed, first_out, out_sem.at[1])
    copy.start()
    outs.append(copy)
    repeat(1, devices, lambda k: count_message(k).wait_send())
    for copy in sends:
        copy.wait_send()
    for copy in outs:
        copy.wait()


def opening(part, gate_params, states, devices, peers):
    own_blocks = part.shape[1]
    tiles = states.shape[0] // ROWS
    planes = ROWS
    per = own_blocks // planes
    f32 = jnp.float32
    chunks = chunk_list(tiles)
    vmem = pl.BlockSpec(memory_space=pltpu.VMEM)
    smem = pl.BlockSpec(memory_space=pltpu.SMEM)
    anywhere = pl.BlockSpec(memory_space=pl.ANY)
    first = chunk_shape(chunks[0], own_blocks)
    own = chunk_shape(chunks[0], planes, per)
    own_next = chunk_shape(chunks[1], planes, per)
    params = (5, (tiles + 1) * ROWS, LANES)
    return pl.pallas_call(
        functools.partial(opening_kernel, devices, peers, own_blocks, chunks),
        out_shape=(
            jax.ShapeDtypeStruct((2 * ROWS, LANES), jnp.int32),
            jax.ShapeDtypeStruct((1,), jnp.int32),
            jax.ShapeDtypeStruct((devices, 1, LANES), jnp.int32),
            jax.ShapeDtypeStruct(params, f32),
            jax.ShapeDtypeStruct(first, f32),
            jax.ShapeDtypeStruct(own_next, f32),
        ),
        in_specs=[vmem] * 6 + [anywhere],
        out_specs=(vmem, smem, vmem, vmem, anywhere, anywhere),
        scratch_shapes=[
            pltpu.VMEM(own, f32),
            pltpu.VMEM(own_next, f32),
            pltpu.VMEM((2 * ROWS, states.shape[1]), f32),
            pltpu.VMEM(first, f32),
            pltpu.VMEM((1, LANES), jnp.int32),
            pltpu.VMEM((devices, 1, LANES), jnp.int32),
            pltpu.SemaphoreType.DMA((PIECES,)),
            pltpu.SemaphoreType.DMA((devices,)),
            pltpu.SemaphoreType.DMA((devices,)),
            pltpu.SemaphoreType.DMA((PIECES, planes)),
            pltpu.SemaphoreType.DMA((PIECES, planes)),
            pltpu.SemaphoreType.DMA((2,)),
        ],
        compiler_params=pltpu.CompilerParams(
            collective_id=0, has_side_effects=True, vmem_limit_bytes=VMEM_LIMIT
        ),
    )(part, *gate_params, states)


def exchange_kernel(peers, own_blocks, chunks, rooms, tables, params, states_ref, ahead, behind, *refs):
    d = my_index(peers)
    plane = plane_of(d, peers)
    depth = depth_of(d, peers)
    planes = ROWS
    depths = peers // 2
    per = own_blocks // planes
    number = len(chunks)
    tiles = chunks[-1][0]
    out, out_row, states, refs = refs[0], refs[1], refs[2], refs[3:]
    owns, refs = (None, behind, *refs[: number - 2]), refs[number - 2 :]
    groups = []
    for _ in range(5):
        groups.append(refs[:number])
        refs = refs[number:]
    landed1, packed2, landed2, packed3, landed3 = groups
    ready, ready_row, send_sem, recv_sem, out_sem, in_sem = refs
    room2, near, room3 = rooms
    wide = planes * P_TABLE // LANES

    def device(to_plane, to_depth):
        return (to_plane // 2, to_depth * 2 + to_plane % 2)

    barrier = pltpu.get_barrier_semaphore()
    partners = [device(plane ^ m, depth) for m in range(1, planes)]
    partners += [device(plane, depth ^ m) for m in range(1, depths)]
    for to in partners:
        pl.semaphore_signal(barrier, inc=1, device_id=to, device_id_type=MESH_ID)
    loads = [
        pltpu.make_async_copy(ahead, landed1[0], in_sem.at[0]),
        pltpu.make_async_copy(
            behind.at[0], landed1[1].at[pl.ds(plane * per, per)], in_sem.at[1]
        ),
        pltpu.make_async_copy(states_ref, states, in_sem.at[2]),
    ]
    for copy in loads:
        copy.start()
    pl.semaphore_wait(barrier, len(partners))

    def gather(c, count, table_row, table_col, src, put, first):
        unroll = 8

        def body(i, _):
            for u in range(unroll):
                k = i * unroll + u
                where = tables[table_row, table_col + k]
                if chunks[c][2] > 1:
                    put[first + k] = src[where]
                else:
                    put[pl.ds(first + k, 1), :] = src[pl.ds(where, 1), :]
            return 0

        lax.fori_loop(0, count // unroll, body, 0)

    def whole(room):
        return -(-room // ROWS) * ROWS

    def message(c, phase, m):
        if phase == 0:
            src = owns[c].at[m]
            dst = landed1[c].at[pl.ds(plane * per, per)]
        elif phase == 1:
            room = near if isinstance(m, int) and m == 1 else room2
            room = room if chunks[c][2] > 1 else whole(room)
            src = packed2[c].at[m - 1, pl.ds(0, room)]
            dst = landed2[c].at[pl.ds(depth * Z_STRIDE, room)]
        else:
            src = packed3[c].at[m - 1, pl.ds(0, room3)]
            dst = landed3[c].at[pl.ds(plane * P_STRIDE, room3)]
        to = device(plane, depth ^ m) if phase == 1 else device(plane ^ m, depth)
        return pltpu.make_async_remote_copy(
            src_ref=src, dst_ref=dst,
            send_sem=send_sem.at[c, phase, m], recv_sem=recv_sem.at[c, phase, m],
            device_id=to, device_id_type=MESH_ID,
        )

    def phase1(c):
        def body(i, _):
            message(c, 0, planes - 1 - i).start()
            return 0

        lax.fori_loop(0, planes - 1, body, 0)

    def keep(tile, value, i, u):
        for c, (t, low, rows) in enumerate(chunks):
            if t == tile and c > 1:
                if rows == 1 and u == 0:
                    landed1[c][pl.ds(plane * per + i, 1), :] = value
                elif rows == 1:
                    owns[c][u, pl.ds(i, 1), :] = value
                elif u == 0:
                    landed1[c][plane * per + i] = value[low : low + rows]
                else:
                    owns[c][u, i] = value[low : low + rows]

    def advance_block(i, u):
        cols = block_columns(i, u)
        spread, slow = spread_of(states, cols)
        total = jnp.zeros((ROWS, LANES), jnp.float32)
        for t in range(1, tiles):
            new, term = gates(states, params, spread, slow, cols, t * ROWS, ROWS)
            keep(t, new, i, u)
            total = total + term
        new_row, term_row = gates(states, params, spread, slow, cols, tiles * ROWS, 1)
        keep(tiles, new_row, i, u)
        new, term = gates(states, params, spread, slow, cols, 0, ROWS)
        total = total + term
        current = jnp.sum(total, axis=0, keepdims=True) + term_row
        moved = states[0:1, cols] - time_step * current
        first = lax.broadcasted_iota(jnp.int32, (ROWS, LANES), 0) == 0
        keep(0, jnp.where(first, jnp.broadcast_to(moved, (ROWS, LANES)), new), i, u)

    def advance_rest():
        loads[2].wait()

        def body(i, _):
            for u in range(planes):
                advance_block(i, u)
            return 0

        lax.fori_loop(0, per, body, 0)

    waited = set()

    def arrive(c, phase, m):
        if (c, phase, m) not in waited:
            waited.add((c, phase, m))
            message(c, phase, m).wait_recv()

    def phase2(c, gate):
        if c < 2:
            loads[c].wait()
        if c:
            repeat(1, planes, lambda m: message(c, 0, m).wait_recv())

        def body(i, _):
            m = depths - 1 - i
            if gate is not None:
                message(gate, 1, m).wait_recv()
            gather(c, whole(room2), depth ^ m, 0, landed1[c], packed2[c].at[m - 1], 0)
            message(c, 1, m).start()
            return 0

        lax.fori_loop(0, depths - 2, body, 0)
        if gate is not None:
            waited.update((gate, 1, m) for m in range(2, depths))
            arrive(gate, 1, 1)
        gather(c, whole(near), depth ^ 1, 0, landed1[c], packed2[c].at[0], 0)
        message(c, 1, 1).start()
        gather(c, whole(near), depth, 0, landed1[c], landed2[c], depth * Z_STRIDE)

    def phase3(c):
        for m in range(1, depths):
            arrive(c, 1, m)

        def body(i, _):
            m = planes - 1 - i
            to = plane ^ m
            gather(
                c, room3, depths + to // 2, (to % 2) * P_TABLE,
                landed2[c], packed3[c].at[m - 1], 0,
            )
            message(c, 2, m).start()
            return 0

        lax.fori_loop(0, planes - 1, body, 0)
        gather(
            c, room3, depths + plane // 2, (plane % 2) * P_TABLE,
            landed2[c], landed3[c], plane * P_STRIDE,
        )

    outs = []

    def finish(c):
        repeat(1, planes, lambda m: message(c, 2, m).wait_recv())
        tile, low, rows = chunks[c]
        first = depths + wide

        def body(i, _):
            for u in range(ROWS):
                b = i * ROWS + u
                where = tables[first + b // LANES, b % LANES]
                if rows > 1:
                    ready[tile, b, low : low + rows] = landed3[c][where]
                else:
                    ready_row[pl.ds(b, 1), :] = landed3[c][pl.ds(where, 1), :]
            return 0

        lax.fori_loop(0, own_blocks // ROWS, body, 0)
        if rows == 1:
            copy = pltpu.make_async_copy(ready_row, out_row, out_sem.at[tile])
        elif low + rows == ROWS:
            copy = pltpu.make_async_copy(ready.at[tile], out.at[tile], out_sem.at[tile])
        else:
            return
        copy.start()
        outs.append(copy)

    for phase, *c in EVENTS:
        (phase1, phase2, phase3, finish, advance_rest)[phase](*c)
    for copy in outs:
        copy.wait()
    for c in range(number):
        if c:
            repeat(1, planes, lambda m: message(c, 0, m).wait_send())
        repeat(1, planes, lambda m: message(c, 2, m).wait_send())
        for m in range(1, depths):
            message(c, 1, m).wait_send()


EVENTS = (
    (0, 1), (1, 0, None), (4,), (0, 2), (0, 3), (1, 1, 0), (2, 0), (1, 2, 1), (0, 4), (2, 1),
    (1, 3, 2), (3, 0), (0, 5), (0, 6), (0, 7), (2, 2), (1, 4, 3), (3, 1), (2, 3), (3, 2),
    (1, 5, 4), (2, 4), (1, 6, 5), (1, 7, None), (3, 3), (2, 5), (3, 4), (2, 6), (2, 7),
    (3, 5), (3, 6), (3, 7),
)


def exchange(tables, params, states, ahead, behind, peers, own_blocks, rooms):
    width = states.shape[0]
    per = own_blocks // ROWS
    planes = ROWS
    depths = peers // 2
    tiles = width // ROWS
    chunks = chunk_list(tiles)
    f32 = jnp.float32

    def buffers(*lead):
        return [pltpu.VMEM(chunk_shape(c, *lead), f32) for c in chunks]

    anywhere = pl.BlockSpec(memory_space=pl.ANY)
    return pl.pallas_call(
        functools.partial(exchange_kernel, peers, own_blocks, chunks, rooms),
        out_shape=(
            jax.ShapeDtypeStruct((tiles, own_blocks, ROWS, LANES), f32),
            jax.ShapeDtypeStruct((own_blocks, LANES), f32),
        ),
        in_specs=[
            pl.BlockSpec(memory_space=pltpu.SMEM),
            pl.BlockSpec(memory_space=pltpu.VMEM),
            anywhere, anywhere, anywhere,
        ],
        out_specs=(anywhere, anywhere),
        scratch_shapes=[
            pltpu.VMEM(states.shape, f32),
            *buffers(planes, per)[2:],
            *buffers(own_blocks),
            *buffers(depths - 1, Z_STRIDE),
            *buffers(depths * Z_STRIDE),
            *buffers(planes - 1, P_STRIDE),
            *buffers(planes * P_STRIDE),
            pltpu.VMEM((tiles, own_blocks, ROWS, LANES), f32),
            pltpu.VMEM((own_blocks, LANES), f32),
            pltpu.SemaphoreType.DMA((len(chunks), 3, planes)),
            pltpu.SemaphoreType.DMA((len(chunks), 3, planes)),
            pltpu.SemaphoreType.DMA((tiles + 1,)),
            pltpu.SemaphoreType.DMA((3,)),
        ],
        compiler_params=pltpu.CompilerParams(
            collective_id=1 + TIERS.index(rooms),
            has_side_effects=True,
            vmem_limit_bytes=VMEM_LIMIT,
        ),
    )(tables, params, states, ahead, behind)


def place_kernel(tiles, blocks, got, got_row, perm, out):
    def body(group, _):
        rows = pl.ds(pl.multiple_of(group * ROWS, ROWS), ROWS)
        orders = perm[rows, :]
        turned = jnp.take_along_axis(
            got_row[rows, :], orders, axis=1, mode="promise_in_bounds"
        )
        for u in range(ROWS):
            b = group * ROWS + u
            cols = pl.ds(pl.multiple_of(b * LANES, LANES), LANES)
            where = jnp.broadcast_to(orders[u : u + 1, :], (ROWS, LANES))
            for t in range(tiles):
                out[t * ROWS : (t + 1) * ROWS, cols] = jnp.take_along_axis(
                    got[t, b], where, axis=1, mode="promise_in_bounds"
                )
            out[tiles * ROWS : tiles * ROWS + 1, cols] = turned[u : u + 1, :]
        return 0

    lax.fori_loop(0, blocks // ROWS, body, 0, unroll=2)


def place(got, got_row, perm, width, own_blocks):
    tiles = got.shape[0]
    step = 64
    return pl.pallas_call(
        functools.partial(place_kernel, tiles, step),
        grid=(own_blocks // step,),
        out_shape=jax.ShapeDtypeStruct((width, own_blocks * LANES), jnp.float32),
        in_specs=[
            pl.BlockSpec((tiles, step, ROWS, LANES), lambda i: (0, i, 0, 0)),
            pl.BlockSpec((step, LANES), lambda i: (i, 0)),
            pl.BlockSpec((step, LANES), lambda i: (i, 0)),
        ],
        out_specs=pl.BlockSpec((width, step * LANES), lambda i: (0, i)),
    )(got, got_row, perm)


def advance(state_rows, half_volt, steepness, gate_rate, conductance, reversal):
    voltage = state_rows[0:1]
    gate_vals = state_rows[1:]
    steady = jax.nn.sigmoid((voltage - half_volt[:, None]) * steepness[:, None])
    damping = jnp.exp(-gate_rate[:, None] * (1.0 + jax.nn.sigmoid(voltage)))
    gate_vals = steady + (gate_vals - steady) * damping
    current = jnp.sum(
        conductance[:, None] * gate_vals * (voltage - reversal[:, None]), axis=0, keepdims=True
    )
    voltage = voltage - time_step * current
    return jnp.concatenate([voltage, gate_vals], axis=0)


def general(counts_all, devices, states, block_part, tile_perm, *gate_params):
    d = lax.axis_index(("group", "peer"))
    local_blocks = block_part.shape[0]
    tile_width = tile_perm.shape[1]
    width = states.shape[0]
    capacity = 2 * local_blocks // devices
    partitions = jnp.arange(devices, dtype=jnp.int32)
    onehot = (block_part[:, None] == partitions[None, :]).astype(jnp.int32)
    if counts_all is None:
        counts_all = lax.all_gather(
            jnp.sum(onehot, axis=0, dtype=jnp.int32), ("group", "peer")
        )
    before = (partitions < d).astype(jnp.int32)
    earlier = jnp.sum(counts_all * before[:, None], axis=0, dtype=jnp.int32)
    rank_in = jnp.sum(
        (jnp.cumsum(onehot, axis=0, dtype=jnp.int32) - onehot) * onehot, axis=1, dtype=jnp.int32
    )
    local_index = jnp.sum(onehot * earlier[None, :], axis=1, dtype=jnp.int32) + rank_in
    slot_index = block_part * capacity + rank_in
    requests = jnp.full((devices * capacity,), -1, jnp.int32).at[slot_index].set(local_index)
    requests = requests.reshape(devices, capacity)
    advanced = advance(states, *gate_params)
    advanced = advanced.reshape(width, local_blocks, tile_width)
    wanted = lax.all_to_all(requests, ("group", "peer"), split_axis=0, concat_axis=0, tiled=True)
    picked = jnp.maximum(wanted, 0).reshape(-1)
    served = jnp.take(advanced, picked, axis=1)
    arrived = lax.all_to_all(
        served.reshape(width, wanted.shape[0], wanted.shape[1], tile_width),
        ("group", "peer"), split_axis=1, concat_axis=1, tiled=True,
    )
    flat_cols = (slot_index[:, None] * tile_width + tile_perm).reshape(-1)
    return jnp.take(arrived.reshape(width, devices * capacity * tile_width), flat_cols, axis=1)


def on_device(devices, peers, states, block_part, tile_perm, *gate_params):
    own_blocks = block_part.shape[0]
    width = states.shape[0]
    if (devices, peers) != (4 * ROWS, ROWS) or width % ROWS != 1:
        return general(None, devices, states, block_part, tile_perm, *gate_params)
    tables, tier, counts, params, ahead, behind = opening(
        block_part.reshape(1, own_blocks), [p.reshape(1, -1) for p in gate_params],
        states, devices, peers,
    )

    def fast(rooms):
        got, got_row = exchange(
            tables, params, states, ahead, behind, peers, own_blocks, rooms
        )
        return place(got, got_row, tile_perm, width, own_blocks)

    def slow():
        matrix = counts[:, 0, :devices]
        return general(matrix, devices, states, block_part, tile_perm, *gate_params)

    choices = [functools.partial(fast, rooms) for rooms in TIERS] + [slow]
    return lax.switch(tier[0], choices)


def solution(mesh):
    both = P(("group", "peer"))
    return jax.shard_map(
        functools.partial(on_device, mesh.devices.size, mesh.shape["peer"]),
        mesh=mesh,
        in_specs=(P(None, ("group", "peer")), both, P(("group", "peer"), None)) + (P(),) * 5,
        out_specs=P(None, ("group", "peer")),
        check_vma=False,
    )
```
